8 devices in a mesh: batch: 2 (over z, y), time: 4 (over x, core).
Axes of the slice: x: 2, y: 2, z: 1, core: 2. Of those that a mesh axis runs over, the one named last changes fastest.
Arguments:
- latent: bfloat16 [16, 4, 96, 768], P(('batch', 'time')), parts along dimension 0
- conv_w: bfloat16 [4, 3, 3, 3, 768, 768], replicated
- conv_b: float32 [4, 768], replicated
- norm_g: float32 [5, 768], replicated
- norm_b: float32 [5, 768], replicated
- attn_w: bfloat16 [4, 768, 768], replicated
- attn_b: float32 [4, 768], replicated
Outputs:
- output: bfloat16 [16, 4, 96, 768], P(('batch', 'time')), parts along dimension 0
There are 2 independent parts. The reference program is written for one: setup_inputs(seed, part) draws one part's arguments, and reference() takes and returns one part's arrays. A program takes and returns all parts, laid end to end along the dimension named above; an argument that names none is the same for every part.
All inputs are finite; a program needn't handle non-finite values.
Results may differ from the reference program's by a relative error of at most 0.0124034.
Values are sent between devices in bfloat16 or wider.
A program may use at most 1 GiB of HBM per device.

```python
import jax
import jax.numpy as jnp
from jax import lax

FRAMES = 8
HEIGHT = 4
WIDTH = 96
CHANNELS = 768
GROUPS = 32
NORM_EPS = 1e-6


def setup_inputs(seed: int = 0, part: int = 0) -> dict:
    part_key = jax.random.fold_in(jax.random.key(seed), part)
    video_keys = jax.random.split(part_key, 4)
    weight_keys = jax.random.split(jax.random.key(seed + 1), 6)
    time_pos = jnp.arange(FRAMES, dtype=jnp.float32) / max(FRAMES - 1, 1) - 0.5
    time_slope = 1.4 + 0.4 * jax.random.uniform(video_keys[0], (), jnp.float32)
    frame_scale = jnp.exp(time_slope * time_pos)[:, None, None, None]
    chan_offset = jax.random.normal(video_keys[1], (CHANNELS,), jnp.float32)
    frame_mean = time_pos[:, None, None, None] * chan_offset
    shared_noise = jax.random.normal(video_keys[2], (1, HEIGHT, WIDTH, CHANNELS), jnp.float32)
    fresh_noise = jax.random.normal(video_keys[3], (FRAMES, HEIGHT, WIDTH, CHANNELS), jnp.float32)
    latent = frame_scale * (0.5 * shared_noise + 0.85 * fresh_noise) + frame_mean
    conv_w = jax.random.normal(weight_keys[0], (4, 3, 3, 3, CHANNELS, CHANNELS), jnp.float32) * (27 * CHANNELS) ** -0.5
    conv_b = 0.3 * jax.random.normal(weight_keys[1], (4, CHANNELS), jnp.float32)
    norm_g = 1.0 + 0.3 * jax.random.normal(weight_keys[2], (5, CHANNELS), jnp.float32)
    norm_b = 0.3 * jax.random.normal(weight_keys[3], (5, CHANNELS), jnp.float32)
    attn_w = jax.random.normal(weight_keys[4], (4, CHANNELS, CHANNELS), jnp.float32) * CHANNELS ** -0.5
    attn_b = 0.3 * jax.random.normal(weight_keys[5], (4, CHANNELS), jnp.float32)
    return {"latent": latent.astype(jnp.bfloat16), "conv_w": conv_w.astype(jnp.bfloat16), "conv_b": conv_b, "norm_g": norm_g, "norm_b": norm_b, "attn_w": attn_w.astype(jnp.bfloat16), "attn_b": attn_b}


def group_norm(feature, norm_gain, norm_shift):
    values_f = feature.astype(jnp.float32)
    grouped = values_f.reshape(FRAMES, HEIGHT, WIDTH, GROUPS, CHANNELS // GROUPS)
    elem_count = FRAMES * HEIGHT * WIDTH * (CHANNELS // GROUPS)
    group_mean = jnp.sum(grouped, axis=(0, 1, 2, 4)) / elem_count
    group_sq = jnp.sum(grouped * grouped, axis=(0, 1, 2, 4)) / elem_count
    inv_std = lax.rsqrt(group_sq - group_mean * group_mean + NORM_EPS)
    mean_full = jnp.repeat(group_mean, CHANNELS // GROUPS)
    scale_full = jnp.repeat(inv_std, CHANNELS // GROUPS) * norm_gain
    return (values_f - mean_full) * scale_full + norm_shift


def causal_conv(activation, kernel, conv_bias):
    padded = jnp.concatenate([activation[:1], activation[:1], activation], axis=0)
    conv_out = lax.conv_general_dilated(padded[None].astype(jnp.float32), kernel.astype(jnp.float32), (1, 1, 1), ((0, 0), (1, 1), (1, 1)), dimension_numbers=("NDHWC", "DHWIO", "NDHWC"))
    return (conv_out[0] + conv_bias).astype(jnp.bfloat16)


def resnet_block(feature, conv_w, conv_b, norm_g, norm_b, norm_first, conv_first):
    activation = jax.nn.silu(group_norm(feature, norm_g[norm_first], norm_b[norm_first])).astype(jnp.bfloat16)
    branch = causal_conv(activation, conv_w[conv_first], conv_b[conv_first])
    activation = jax.nn.silu(group_norm(branch, norm_g[norm_first + 1], norm_b[norm_first + 1])).astype(jnp.bfloat16)
    branch = causal_conv(activation, conv_w[conv_first + 1], conv_b[conv_first + 1])
    return (feature.astype(jnp.float32) + branch.astype(jnp.float32)).astype(jnp.bfloat16)


def spatial_attention(feature, norm_gain, norm_shift, attn_w, attn_b):
    normed = group_norm(feature, norm_gain, norm_shift).astype(jnp.bfloat16)
    tokens = normed.reshape(FRAMES, HEIGHT * WIDTH, CHANNELS)
    score_scale = CHANNELS ** -0.5

    def one_frame(frame_tok):
        queries = (jnp.dot(frame_tok, attn_w[0], preferred_element_type=jnp.float32) + attn_b[0]).astype(jnp.bfloat16)
        keys_t = (jnp.dot(frame_tok, attn_w[1], preferred_element_type=jnp.float32) + attn_b[1]).astype(jnp.bfloat16)
        values_t = (jnp.dot(frame_tok, attn_w[2], preferred_element_type=jnp.float32) + attn_b[2]).astype(jnp.bfloat16)
        scores = jnp.dot(queries, keys_t.T, preferred_element_type=jnp.float32) * score_scale
        attn_probs = jax.nn.softmax(scores, axis=-1).astype(jnp.bfloat16)
        mixed_val = jnp.dot(attn_probs, values_t, preferred_element_type=jnp.float32).astype(jnp.bfloat16)
        return (jnp.dot(mixed_val, attn_w[3], preferred_element_type=jnp.float32) + attn_b[3]).astype(jnp.bfloat16)

    projected = lax.map(one_frame, tokens).reshape(feature.shape)
    return (feature.astype(jnp.float32) + projected.astype(jnp.float32)).astype(jnp.bfloat16)


def reference(latent, conv_w, conv_b, norm_g, norm_b, attn_w, attn_b):
    feature = resnet_block(latent, conv_w, conv_b, norm_g, norm_b, 0, 0)
    feature = spatial_attention(feature, norm_g[2], norm_b[2], attn_w, attn_b)
    return resnet_block(feature, conv_w, conv_b, norm_g, norm_b, 3, 2)
```

```python
import jax
import jax.numpy as jnp
from jax import lax
from jax.experimental import pallas as pl
from jax.experimental.pallas import tpu as pltpu
from jax.sharding import PartitionSpec as P

GROUPS = 32
NORM_EPS = 1e-6
MESH = pl.DeviceIdType.MESH
BF = jnp.bfloat16
F32 = jnp.float32
RING = 4


def make_kernel(group_size, height, width, channels):
    C = channels
    NT = C // 256
    FR = height * width
    assert height == 4
    elem_count = float(group_size * 2 * FR * (C // GROUPS))
    units_conv = 3 * NT
    units_all = 4 * units_conv

    def body(latent, conv_w, conv_b, norm_g, norm_b, attn_w, attn_b, gmask, out,
             wbuf, awbuf, xs, xres, hbuf, halo, acc, qkv, stat, norm,
             wsem, awsem, insem, outsem, hsend, hrecv, ssend, srecv):
        me = lax.axis_index("time")

        def weight_copies(u):
            conv = u // units_conv
            rest = lax.rem(u, units_conv)
            tap_t = 2 - rest // NT
            tile = lax.rem(rest, NT)
            slot = lax.rem(u, RING)
            return [pltpu.make_async_copy(
                conv_w.at[conv, tap_t, d, :, :, pl.ds(pl.multiple_of(tile * 256, 256), 256)],
                wbuf.at[slot, d], wsem.at[slot, d]) for d in range(3)]

        def attn_weight_copy():
            return pltpu.make_async_copy(attn_w, awbuf, awsem)

        def in_copy(n):
            return pltpu.make_async_copy(latent.at[:, pl.ds(n * 256, 256)], xres.at[n], insem.at[n])

        def out_copy(n):
            return pltpu.make_async_copy(xres.at[n], out.at[:, pl.ds(n * 256, 256)], outsem.at[n])

        def halo_copy(src, conv, n, f):
            return pltpu.make_async_remote_copy(
                src_ref=src.at[n, pl.ds(f * FR, FR)],
                dst_ref=halo.at[conv, n, pl.ds(f * FR, FR)],
                send_sem=hsend.at[conv, n, f], recv_sem=hrecv.at[conv, n, f],
                device_id={"time": lax.rem(me + 1, group_size)}, device_id_type=MESH)

        def halo_start(src, conv, n):
            @pl.when(me < group_size - 1)
            def _():
                for f in (1, 0):
                    halo_copy(src, conv, n, f).start()

        def halo_wait_send(src, conv):
            @pl.when(me < group_size - 1)
            def _():
                for n in range(NT):
                    for f in (1, 0):
                        halo_copy(src, conv, n, f).wait_send()

        def stat_copy(g, p):
            return pltpu.make_async_remote_copy(
                src_ref=stat.at[g, me], dst_ref=stat.at[g, me],
                send_sem=ssend.at[g, p], recv_sem=srecv.at[g, p],
                device_id={"time": lax.rem(me + p, group_size)}, device_id_type=MESH)

        for n in range(NT):
            in_copy(n).start()
        for u in range(RING):
            for c in weight_copies(u):
                c.start()
        attn_weight_copy().start()

        barrier = pltpu.get_barrier_semaphore()
        for p in range(1, group_size):
            pl.semaphore_signal(barrier, inc=1, device_id={"time": lax.rem(me + p, group_size)}, device_id_type=MESH)

        def tile_cols(n):
            return pl.ds(n * 256 if isinstance(n, int) else pl.multiple_of(n * 256, 256), 256)

        def put_stats(g, n, s1, s2):
            stat[g, me, 0:1, tile_cols(n)] = jnp.sum(s1, axis=0, keepdims=True)
            stat[g, me, 1:2, tile_cols(n)] = jnp.sum(s2, axis=0, keepdims=True)

        def fold(v):
            return jnp.sum(v.reshape(v.shape[0] // 8, 8, v.shape[1]), axis=0)

        def exchange(g):
            for p in range(1, group_size):
                stat_copy(g, p).start()
            for p in range(1, group_size):
                stat_copy(g, p).wait_recv()
            total = stat[g, 0]
            for r in range(1, group_size):
                total = total + stat[g, r]
            for p in range(1, group_size):
                stat_copy(g, p).wait_send()

            def left(v, k):
                return pltpu.roll(v, C - k, 1)

            s = total + left(total, 1)
            s = s + left(s, 2)
            s = s + left(s, 4)
            s = s + left(s, 8) + left(s, 16)
            s = jnp.where(gmask[...] > 0.5, s, 0.0)
            s = s + pltpu.roll(s, 1, 1)
            s = s + pltpu.roll(s, 2, 1)
            s = s + pltpu.roll(s, 4, 1)
            s = s + pltpu.roll(s, 8, 1) + pltpu.roll(s, 16, 1)
            mean = s[0:1] / elem_count
            var = s[1:2] / elem_count - mean * mean
            norm[0:1] = mean
            norm[1:2] = lax.rsqrt(var + NORM_EPS) * norm_g[pl.ds(g, 1)]
            norm[2:3] = norm_b[pl.ds(g, 1)]

        def normed(v, k):
            cols = pl.ds(k * 256, 256)
            return (v.astype(F32) - norm[0:1, cols]) * norm[1:2, cols] + norm[2:3, cols]

        row_id = lax.broadcasted_iota(jnp.int32, (width, 256), 0)

        def activate(src, frame_slot, f, row):
            at = pl.ds(pl.multiple_of((frame_slot * height + row) * width, width), width)
            for k in range(NT):
                z = normed(src[k, pl.ds(pl.multiple_of((f * height + row) * width, width), width), :], k)
                z = z * lax.logistic(z)
                xs[at, C + k * 256:C + (k + 1) * 256] = z.astype(BF)
                xs[at, k * 256:(k + 1) * 256] = jnp.where(row_id == 0, 0.0, pltpu.roll(z, 1, 0)).astype(BF)
                xs[at, 2 * C + k * 256:2 * C + (k + 1) * 256] = jnp.where(row_id == width - 1, 0.0, pltpu.roll(z, width - 1, 0)).astype(BF)

        def trip(slot, tap_t, n):
            for d in (1, 0, 2):
                w = wbuf[slot, d].reshape(3 * C, 256)
                if d == 1:
                    lhs = xs[pl.ds(pl.multiple_of(tap_t * FR, FR), 2 * FR), :]
                    acc[n] += jnp.dot(lhs, w, preferred_element_type=F32)
                else:
                    tall = FR - width
                    lo, dst = (0, width) if d == 0 else (width, 0)
                    lhs = jnp.concatenate([xs[pl.ds(pl.multiple_of((tap_t + f) * FR, FR) + lo, tall), :] for f in range(2)], axis=0)
                    r = jnp.dot(lhs, w, preferred_element_type=F32)
                    for f in range(2):
                        acc[n, f * FR + dst:f * FR + dst + tall, :] += r[f * tall:(f + 1) * tall]

        def epilogue(conv, n, g):
            bias = conv_b[pl.ds(conv, 1), tile_cols(n)]

            def rows_out(j, carry):
                rows = pl.ds(pl.multiple_of(j * width, width), width)
                h = (acc[n, rows, :] + bias).astype(BF)
                acc[n, rows, :] = jnp.zeros((width, 256), F32)
                if conv % 2 == 0:
                    hbuf[n, rows, :] = h
                else:
                    h = (xres[n, rows, :].astype(F32) + h.astype(F32)).astype(BF)
                    xres[n, rows, :] = h
                if g is None:
                    return carry
                hf = h.astype(F32)
                return carry[0] + fold(hf), carry[1] + fold(hf * hf)

            s1, s2 = lax.fori_loop(0, 2 * height, rows_out, (jnp.zeros((8, 256), F32), jnp.zeros((8, 256), F32)))
            if g is not None:
                put_stats(g, n, s1, s2)

        def conv(c, src, g_out):
            base = c * units_conv

            def own_rows(j, carry):
                activate(src, 2 + j // height, j // height, lax.rem(j, height))
                return carry

            lax.fori_loop(0, 2 * height, own_rows, 0)

            def get_halo(f):
                @pl.when(me == 0)
                def _():
                    def copy_row(j, carry):
                        xs[pl.ds(pl.multiple_of((f * height + j) * width, width), width), :] = (
                            xs[pl.ds(pl.multiple_of((2 * height + j) * width, width), width), :])
                        return carry
                    lax.fori_loop(0, height, copy_row, 0)

                @pl.when(me > 0)
                def _():
                    for n in range(NT):
                        halo_copy(src, c, n, f).wait_recv()

                    def halo_rows(j, carry):
                        activate(halo.at[c], f, f, j)
                        return carry

                    lax.fori_loop(0, height, halo_rows, 0)

            def step(t, carry):
                @pl.when(t == NT)
                def _():
                    get_halo(1)

                @pl.when(t == 2 * NT)
                def _():
                    get_halo(0)
                    halo_wait_send(src, c)

                u = base + t
                n = lax.rem(t, NT)
                for w in weight_copies(u):
                    w.wait()
                trip(lax.rem(u, RING), 2 - t // NT, n)

                @pl.when(u + RING < units_all)
                def _():
                    for w in weight_copies(u + RING):
                        w.start()

                @pl.when(t >= 2 * NT)
                def _():
                    epilogue(c, n, g_out)
                    if c % 2 == 0:
                        halo_start(hbuf, c + 1, n)
                return carry

            lax.fori_loop(0, 3 * NT, step, 0)

        def attention(g):
            def rows_norm(j, carry):
                at = pl.ds(pl.multiple_of(j * width, width), width)
                for k in range(NT):
                    xs[at, k * 256:(k + 1) * 256] = normed(xres[k, at, :], k).astype(BF)
                return carry

            lax.fori_loop(0, 2 * height, rows_norm, 0)
            attn_weight_copy().wait()
            for w in range(3):
                for n in range(NT):
                    cols = slice(n * 256, (n + 1) * 256)
                    v = jnp.dot(xs[0:2 * FR, 0:C], awbuf[w, :, cols], preferred_element_type=F32) + attn_b[w:w + 1, cols]
                    qkv[w, :, cols] = v.astype(BF)
            for f in range(2):
                rows = slice(f * FR, (f + 1) * FR)
                scores = lax.dot_general(qkv[0, rows, :], qkv[1, rows, :], (((1,), (1,)), ((), ())), preferred_element_type=F32)
                scores = scores * (C ** -0.5)
                e = jnp.exp(scores - jnp.max(scores, axis=1, keepdims=True))
                probs = (e / jnp.sum(e, axis=1, keepdims=True)).astype(BF)
                xs[rows, C:2 * C] = jnp.dot(probs, qkv[2, rows, :], preferred_element_type=F32).astype(BF)
            for n in range(NT):
                cols = slice(n * 256, (n + 1) * 256)
                h = (jnp.dot(xs[0:2 * FR, C:2 * C], awbuf[3, :, cols], preferred_element_type=F32) + attn_b[3:4, cols]).astype(BF)
                h = (xres[n].astype(F32) + h.astype(F32)).astype(BF)
                xres[n] = h
                hf = h.astype(F32)
                put_stats(g + 1, n, fold(hf), fold(hf * hf))
                halo_start(xres, 2, n)

        for n in range(NT):
            acc[n] = jnp.zeros((2 * FR, 256), F32)
        for g in range(5):
            stat[g, me] = jnp.zeros((8, C), F32)
        for n in range(NT):
            in_copy(n).wait()
        pl.semaphore_wait(barrier, group_size - 1)
        for n in range(NT):
            halo_start(xres, 0, n)
        for n in range(NT):
            def in_stats(j, carry):
                v = xres[n, pl.ds(pl.multiple_of(j * width, width), width), :].astype(F32)
                return carry[0] + fold(v), carry[1] + fold(v * v)

            s1, s2 = lax.fori_loop(0, 2 * height, in_stats, (jnp.zeros((8, 256), F32), jnp.zeros((8, 256), F32)))
            put_stats(0, n, s1, s2)
        exchange(0)
        conv(0, xres, 1)
        exchange(1)
        conv(1, hbuf, 2)
        exchange(2)
        attention(2)
        exchange(3)
        conv(2, xres, 4)
        exchange(4)
        conv(3, hbuf, None)
        for n in range(NT):
            out_copy(n).start()
        for n in range(NT):
            out_copy(n).wait()

    scratch = [
        pltpu.VMEM((RING, 3, 3, C, 256), BF),
        pltpu.VMEM((4, C, C), BF),
        pltpu.VMEM((4 * FR, 3 * C), BF),
        pltpu.VMEM((NT, 2 * FR, 256), BF),
        pltpu.VMEM((NT, 2 * FR, 256), BF),
        pltpu.VMEM((4, NT, 2 * FR, 256), BF),
        pltpu.VMEM((NT, 2 * FR, 256), F32),
        pltpu.VMEM((3, 2 * FR, C), BF),
        pltpu.VMEM((5, group_size, 8, C), F32),
        pltpu.VMEM((8, C), F32),
        pltpu.SemaphoreType.DMA((RING, 3)),
        pltpu.SemaphoreType.DMA,
        pltpu.SemaphoreType.DMA((NT,)),
        pltpu.SemaphoreType.DMA((NT,)),
        pltpu.SemaphoreType.DMA((4, NT, 2)),
        pltpu.SemaphoreType.DMA((4, NT, 2)),
        pltpu.SemaphoreType.DMA((5, group_size)),
        pltpu.SemaphoreType.DMA((5, group_size)),
    ]
    return body, scratch


def solution(mesh):
    group_size = mesh.shape["time"]
    video_spec = P(("batch", "time"), None, None, None)

    def device_body(latent, conv_w, conv_b, norm_g, norm_b, attn_w, attn_b):
        frames, height, width, channels = latent.shape
        body, scratch = make_kernel(group_size, height, width, channels)
        gmask = jnp.broadcast_to((jnp.arange(channels) % (channels // GROUPS) == 0).astype(F32), (8, channels))
        hbm = pl.BlockSpec(memory_space=pltpu.HBM)
        vmem = pl.BlockSpec(memory_space=pltpu.VMEM)
        out = pl.pallas_call(
            body,
            out_shape=jax.ShapeDtypeStruct((frames * height * width, channels), BF),
            in_specs=[hbm, hbm, vmem, vmem, vmem, hbm, vmem, vmem],
            out_specs=hbm,
            scratch_shapes=scratch,
            compiler_params=pltpu.CompilerParams(collective_id=0, has_side_effects=True, vmem_limit_bytes=60 * 1024 * 1024),
            name="mid_block",
        )(latent.reshape(frames * height * width, channels), conv_w, conv_b, norm_g, norm_b, attn_w, attn_b, gmask)
        return out.reshape(latent.shape)

    return jax.shard_map(device_body, mesh=mesh, in_specs=(video_spec, P(), P(), P(), P(), P(), P()), out_specs=video_spec, check_vma=False)
```

```python
import jax
import jax.numpy as jnp
from jax import lax
from jax.experimental import pallas as pl
from jax.experimental.pallas import tpu as pltpu
from jax.sharding import PartitionSpec as P

GROUPS = 32
NORM_EPS = 1e-6
MESH = pl.DeviceIdType.MESH
BF = jnp.bfloat16
F32 = jnp.float32
RING = 4


def make_kernel(group_size, height, width, channels):
    C = channels
    NT = C // 256
    FR = height * width
    assert height == 4
    elem_count = float(group_size * 2 * FR * (C // GROUPS))
    units_conv = 3 * NT
    units_all = 4 * units_conv

    def body(latent, conv_w, conv_b, norm_g, norm_b, attn_w, attn_b, out,
             wbuf, awbuf, xs, xres, hbuf, halo, acc, qkv, stat, norm,
             wsem, awsem, insem, outsem, hsend, hrecv, ssend, srecv):
        me = lax.axis_index("time")

        def weight_copies(u):
            conv = u // units_conv
            rest = lax.rem(u, units_conv)
            tap_t = 2 - rest // NT
            tile = lax.rem(rest, NT)
            slot = lax.rem(u, RING)
            return [pltpu.make_async_copy(
                conv_w.at[conv, tap_t, d, :, :, pl.ds(pl.multiple_of(tile * 256, 256), 256)],
                wbuf.at[slot, d], wsem.at[slot, d]) for d in range(3)]

        def attn_weight_copy():
            return pltpu.make_async_copy(attn_w, awbuf, awsem)

        def in_copy(n):
            return pltpu.make_async_copy(latent.at[:, pl.ds(n * 256, 256)], xres.at[n], insem.at[n])

        def out_copy(n):
            return pltpu.make_async_copy(xres.at[n], out.at[:, pl.ds(n * 256, 256)], outsem.at[n])

        def halo_copy(src, conv, n, f):
            return pltpu.make_async_remote_copy(
                src_ref=src.at[n, pl.ds(f * FR, FR)],
                dst_ref=halo.at[conv, n, pl.ds(f * FR, FR)],
                send_sem=hsend.at[conv, n, f], recv_sem=hrecv.at[conv, n, f],
                device_id={"time": lax.rem(me + 1, group_size)}, device_id_type=MESH)

        def halo_start(src, conv):
            @pl.when(me < group_size - 1)
            def _():
                for f in (1, 0):
                    for n in range(NT):
                        halo_copy(src, conv, n, f).start()

        def halo_wait_send(src, conv):
            @pl.when(me < group_size - 1)
            def _():
                for n in range(NT):
                    for f in (1, 0):
                        halo_copy(src, conv, n, f).wait_send()

        def stat_copy(g, p):
            return pltpu.make_async_remote_copy(
                src_ref=stat.at[g, me], dst_ref=stat.at[g, me],
                send_sem=ssend.at[g, p], recv_sem=srecv.at[g, p],
                device_id={"time": lax.rem(me + p, group_size)}, device_id_type=MESH)

        for n in range(NT):
            in_copy(n).start()
        for u in range(RING):
            for c in weight_copies(u):
                c.start()
        attn_weight_copy().start()

        barrier = pltpu.get_barrier_semaphore()
        for p in range(1, group_size):
            pl.semaphore_signal(barrier, inc=1, device_id={"time": lax.rem(me + p, group_size)}, device_id_type=MESH)

        def tile_cols(n):
            return pl.ds(n * 256 if isinstance(n, int) else pl.multiple_of(n * 256, 256), 256)

        def put_stats(g, n, s1, s2):
            stat[g, me, 0:1, tile_cols(n)] = jnp.sum(s1, axis=0, keepdims=True)
            stat[g, me, 1:2, tile_cols(n)] = jnp.sum(s2, axis=0, keepdims=True)

        def fold(v):
            return jnp.sum(v.reshape(v.shape[0] // 8, 8, v.shape[1]), axis=0)

        lane = lax.broadcasted_iota(jnp.int32, (8, 128), 1)

        def group_totals(v):
            size = C // GROUPS
            parts = [v[:, i * 128:(i + 1) * 128] for i in range(C // 128)]
            done = [jnp.zeros((8, 128), F32) for _ in parts]
            for q in range(GROUPS):
                lo, hi = q * size, (q + 1) * size
                inside = [(i, (lane >= lo - i * 128) & (lane < hi - i * 128)) for i in range(lo // 128, (hi - 1) // 128 + 1)]
                picked = sum(jnp.where(m, parts[i], 0.0) for i, m in inside)
                total = jnp.sum(picked, axis=1, keepdims=True)
                for i, m in inside:
                    done[i] = jnp.where(m, total, done[i])
            return jnp.concatenate(done, axis=1)

        def exchange(g, then=None):
            for p in range(1, group_size):
                stat_copy(g, p).start()
            if then is not None:
                then()
            for p in range(1, group_size):
                stat_copy(g, p).wait_recv()
            total = stat[g, 0]
            for r in range(1, group_size):
                total = total + stat[g, r]
            for p in range(1, group_size):
                stat_copy(g, p).wait_send()
            s = group_totals(total)
            mean = s[0:1] / elem_count
            var = s[1:2] / elem_count - mean * mean
            norm[0:1] = mean
            norm[1:2] = lax.rsqrt(var + NORM_EPS) * norm_g[pl.ds(g, 1)]
            norm[2:3] = norm_b[pl.ds(g, 1)]

        def normed(v, k):
            cols = pl.ds(k * 256, 256)
            return (v.astype(F32) - norm[0:1, cols]) * norm[1:2, cols] + norm[2:3, cols]

        row_id = lax.broadcasted_iota(jnp.int32, (width, 256), 0)

        def activate(src, frame_slot, f, row):
            at = pl.ds(pl.multiple_of((frame_slot * height + row) * width, width), width)
            for k in range(NT):
                z = normed(src[k, pl.ds(pl.multiple_of((f * height + row) * width, width), width), :], k)
                z = z * lax.logistic(z)
                xs[at, C + k * 256:C + (k + 1) * 256] = z.astype(BF)
                xs[at, k * 256:(k + 1) * 256] = jnp.where(row_id == 0, 0.0, pltpu.roll(z, 1, 0)).astype(BF)
                xs[at, 2 * C + k * 256:2 * C + (k + 1) * 256] = jnp.where(row_id == width - 1, 0.0, pltpu.roll(z, width - 1, 0)).astype(BF)

        def trip(slot, tap_t, n):
            for d in (1, 0, 2):
                w = wbuf[slot, d].reshape(3 * C, 256)
                if d == 1:
                    lhs = xs[pl.ds(pl.multiple_of(tap_t * FR, FR), 2 * FR), :]
                    acc[n] += jnp.dot(lhs, w, preferred_element_type=F32)
                else:
                    tall = FR - width
                    lo, dst = (0, width) if d == 0 else (width, 0)
                    lhs = jnp.concatenate([xs[pl.ds(pl.multiple_of((tap_t + f) * FR, FR) + lo, tall), :] for f in range(2)], axis=0)
                    r = jnp.dot(lhs, w, preferred_element_type=F32)
                    for f in range(2):
                        acc[n, f * FR + dst:f * FR + dst + tall, :] += r[f * tall:(f + 1) * tall]

        def epilogue(conv, n, g):
            bias = conv_b[pl.ds(conv, 1), tile_cols(n)]

            def rows_out(j, carry):
                rows = pl.ds(pl.multiple_of(j * width, width), width)
                h = (acc[n, rows, :] + bias).astype(BF)
                acc[n, rows, :] = jnp.zeros((width, 256), F32)
                if conv % 2 == 0:
                    hbuf[n, rows, :] = h
                else:
                    h = (xres[n, rows, :].astype(F32) + h.astype(F32)).astype(BF)
                    xres[n, rows, :] = h
                if g is None:
                    return carry
                hf = h.astype(F32)
                return carry[0] + fold(hf), carry[1] + fold(hf * hf)

            s1, s2 = lax.fori_loop(0, 2 * height, rows_out, (jnp.zeros((8, 256), F32), jnp.zeros((8, 256), F32)))
            if g is not None:
                put_stats(g, n, s1, s2)

        def conv(c, src, g_out):
            base = c * units_conv

            def own_rows(j, carry):
                activate(src, 2 + j // height, j // height, lax.rem(j, height))
                return carry

            lax.fori_loop(0, 2 * height, own_rows, 0)

            def get_halo(f):
                @pl.when(me == 0)
                def _():
                    def copy_row(j, carry):
                        xs[pl.ds(pl.multiple_of((f * height + j) * width, width), width), :] = (
                            xs[pl.ds(pl.multiple_of((2 * height + j) * width, width), width), :])
                        return carry
                    lax.fori_loop(0, height, copy_row, 0)

                @pl.when(me > 0)
                def _():
                    for n in range(NT):
                        halo_copy(src, c, n, f).wait_recv()

                    def halo_rows(j, carry):
                        activate(halo.at[c], f, f, j)
                        return carry

                    lax.fori_loop(0, height, halo_rows, 0)

            def step(t, carry):
                @pl.when(t == NT)
                def _():
                    get_halo(1)

                @pl.when(t == 2 * NT)
                def _():
                    get_halo(0)
                    halo_wait_send(src, c)

                u = base + t
                n = lax.rem(t, NT)
                for w in weight_copies(u):
                    w.wait()
                trip(lax.rem(u, RING), 2 - t // NT, n)

                @pl.when(u + RING < units_all)
                def _():
                    for w in weight_copies(u + RING):
                        w.start()

                @pl.when(t >= 2 * NT)
                def _():
                    epilogue(c, n, g_out)
                return carry

            lax.fori_loop(0, 3 * NT, step, 0)

        def attention(g):
            def rows_norm(j, carry):
                at = pl.ds(pl.multiple_of(j * width, width), width)
                for k in range(NT):
                    xs[at, k * 256:(k + 1) * 256] = normed(xres[k, at, :], k).astype(BF)
                return carry

            lax.fori_loop(0, 2 * height, rows_norm, 0)
            attn_weight_copy().wait()
            for w in range(3):
                for n in range(NT):
                    cols = slice(n * 256, (n + 1) * 256)
                    v = jnp.dot(xs[0:2 * FR, 0:C], awbuf[w, :, cols], preferred_element_type=F32) + attn_b[w:w + 1, cols]
                    qkv[w, :, cols] = v.astype(BF)
            for f in range(2):
                rows = slice(f * FR, (f + 1) * FR)
                scores = lax.dot_general(qkv[0, rows, :], qkv[1, rows, :], (((1,), (1,)), ((), ())), preferred_element_type=F32)
                scores = scores * (C ** -0.5)
                e = jnp.exp(scores - jnp.max(scores, axis=1, keepdims=True))
                probs = (e / jnp.sum(e, axis=1, keepdims=True)).astype(BF)
                xs[rows, C:2 * C] = jnp.dot(probs, qkv[2, rows, :], preferred_element_type=F32).astype(BF)
            for n in range(NT):
                cols = slice(n * 256, (n + 1) * 256)
                h = (jnp.dot(xs[0:2 * FR, C:2 * C], awbuf[3, :, cols], preferred_element_type=F32) + attn_b[3:4, cols]).astype(BF)
                h = (xres[n].astype(F32) + h.astype(F32)).astype(BF)
                xres[n] = h
                hf = h.astype(F32)
                put_stats(g + 1, n, fold(hf), fold(hf * hf))

        for n in range(NT):
            acc[n] = jnp.zeros((2 * FR, 256), F32)
        for g in range(5):
            stat[g, me] = jnp.zeros((8, C), F32)
        for n in range(NT):
            in_copy(n).wait()
        pl.semaphore_wait(barrier, group_size - 1)
        for n in range(NT):
            def in_stats(j, carry):
                v = xres[n, pl.ds(pl.multiple_of(j * width, width), width), :].astype(F32)
                return carry[0] + fold(v), carry[1] + fold(v * v)

            s1, s2 = lax.fori_loop(0, 2 * height, in_stats, (jnp.zeros((8, 256), F32), jnp.zeros((8, 256), F32)))
            put_stats(0, n, s1, s2)
        exchange(0, lambda: halo_start(xres, 0))
        conv(0, xres, 1)
        exchange(1, lambda: halo_start(hbuf, 1))
        conv(1, hbuf, 2)
        exchange(2)
        attention(2)
        exchange(3, lambda: halo_start(xres, 2))
        conv(2, xres, 4)
        exchange(4, lambda: halo_start(hbuf, 3))
        conv(3, hbuf, None)
        for n in range(NT):
            out_copy(n).start()
        for n in range(NT):
            out_copy(n).wait()

    scratch = [
        pltpu.VMEM((RING, 3, 3, C, 256), BF),
        pltpu.VMEM((4, C, C), BF),
        pltpu.VMEM((4 * FR, 3 * C), BF),
        pltpu.VMEM((NT, 2 * FR, 256), BF),
        pltpu.VMEM((NT, 2 * FR, 256), BF),
        pltpu.VMEM((4, NT, 2 * FR, 256), BF),
        pltpu.VMEM((NT, 2 * FR, 256), F32),
        pltpu.VMEM((3, 2 * FR, C), BF),
        pltpu.VMEM((5, group_size, 8, C), F32),
        pltpu.VMEM((8, C), F32),
        pltpu.SemaphoreType.DMA((RING, 3)),
        pltpu.SemaphoreType.DMA,
        pltpu.SemaphoreType.DMA((NT,)),
        pltpu.SemaphoreType.DMA((NT,)),
        pltpu.SemaphoreType.DMA((4, NT, 2)),
        pltpu.SemaphoreType.DMA((4, NT, 2)),
        pltpu.SemaphoreType.DMA((5, group_size)),
        pltpu.SemaphoreType.DMA((5, group_size)),
    ]
    return body, scratch


def solution(mesh):
    group_size = mesh.shape["time"]
    video_spec = P(("batch", "time"), None, None, None)

    def device_body(latent, conv_w, conv_b, norm_g, norm_b, attn_w, attn_b):
        frames, height, width, channels = latent.shape
        body, scratch = make_kernel(group_size, height, width, channels)
        hbm = pl.BlockSpec(memory_space=pltpu.HBM)
        vmem = pl.BlockSpec(memory_space=pltpu.VMEM)
        out = pl.pallas_call(
            body,
            out_shape=jax.ShapeDtypeStruct((frames * height * width, channels), BF),
            in_specs=[hbm, hbm, vmem, vmem, vmem, hbm, vmem],
            out_specs=hbm,
            scratch_shapes=scratch,
            compiler_params=pltpu.CompilerParams(collective_id=0, has_side_effects=True, vmem_limit_bytes=60 * 1024 * 1024),
            name="mid_block",
        )(latent.reshape(frames * height * width, channels), conv_w, conv_b, norm_g, norm_b, attn_w, attn_b)
        return out.reshape(latent.shape)

    return jax.shard_map(device_body, mesh=mesh, in_specs=(video_spec, P(), P(), P(), P(), P(), P()), out_specs=video_spec, check_vma=False)
```

```python
import jax
import jax.numpy as jnp
from jax import lax
from jax.experimental import pallas as pl
from jax.experimental.pallas import tpu as pltpu
from jax.sharding import PartitionSpec as P

GROUPS = 32
NORM_EPS = 1e-6
MESH = pl.DeviceIdType.MESH
BF = jnp.bfloat16
F32 = jnp.float32
RING = 6


def make_kernel(group_size, height, width, channels):
    C = channels
    NT = C // 256
    FR = height * width
    assert height == 4
    elem_count = float(group_size * 2 * FR * (C // GROUPS))
    units_conv = 3 * NT
    units_all = 4 * units_conv

    def body(latent, conv_w, conv_b, norm_g, norm_b, attn_w, attn_b, out,
             wbuf, awbuf, xs0, xs1, xs2, xs3, buf, halo, acc, qkv, stat, norm,
             wsem, awsem, insem, outsem, hsend, hrecv, ssend, srecv):
        me = lax.axis_index("time")
        xs = (xs0, xs1, xs2, xs3)
        xres = buf.at[0]

        def weight_copies(u):
            conv = u // units_conv
            rest = lax.rem(u, units_conv)
            tap_t = 2 - rest // NT
            tile = lax.rem(rest, NT)
            slot = lax.rem(u, RING)
            return [pltpu.make_async_copy(
                conv_w.at[conv, tap_t, d, :, :, pl.ds(pl.multiple_of(tile * 256, 256), 256)],
                wbuf.at[slot, d], wsem.at[slot, d]) for d in range(3)]

        def attn_weight_copy():
            return pltpu.make_async_copy(attn_w, awbuf, awsem)

        def in_copy(n):
            return pltpu.make_async_copy(latent.at[:, pl.ds(n * 256, 256)], xres.at[n], insem.at[n])

        def out_copy(n):
            return pltpu.make_async_copy(xres.at[n], out.at[:, pl.ds(n * 256, 256)], outsem.at[n])

        def halo_copy(conv, n, f):
            return pltpu.make_async_remote_copy(
                src_ref=buf.at[lax.rem(conv, 2), n, pl.ds(f * FR, FR)],
                dst_ref=halo.at[conv, n, pl.ds(f * FR, FR)],
                send_sem=hsend.at[conv, n, f], recv_sem=hrecv.at[conv, n, f],
                device_id={"time": lax.rem(me + 1, group_size)}, device_id_type=MESH)

        def first_copy(conv, n, f):
            return pltpu.make_async_copy(
                buf.at[lax.rem(conv, 2), n, pl.ds(0, FR)], halo.at[conv, n, pl.ds(f * FR, FR)], hrecv.at[conv, n, f])

        def halo_start(conv):
            @pl.when(me < group_size - 1)
            def _():
                for f in (1, 0):
                    for n in range(NT):
                        halo_copy(conv, n, f).start()

            @pl.when(me == 0)
            def _():
                for f in (1, 0):
                    for n in range(NT):
                        first_copy(conv, n, f).start()

        def halo_wait(conv, f):
            @pl.when(me == 0)
            def _():
                for n in range(NT):
                    first_copy(conv, n, f).wait()

            @pl.when(me > 0)
            def _():
                for n in range(NT):
                    halo_copy(conv, n, f).wait_recv()

        def halo_wait_send(conv):
            @pl.when(me < group_size - 1)
            def _():
                for n in range(NT):
                    for f in (1, 0):
                        halo_copy(conv, n, f).wait_send()

        def stat_copy(g, p):
            return pltpu.make_async_remote_copy(
                src_ref=stat.at[g, me], dst_ref=stat.at[g, me],
                send_sem=ssend.at[g, p], recv_sem=srecv.at[g, p],
                device_id={"time": lax.rem(me + p, group_size)}, device_id_type=MESH)

        for n in range(NT):
            in_copy(n).start()
        for u in range(RING):
            for c in weight_copies(u):
                c.start()
        attn_weight_copy().start()

        barrier = pltpu.get_barrier_semaphore()
        for p in range(1, group_size):
            pl.semaphore_signal(barrier, inc=1, device_id={"time": lax.rem(me + p, group_size)}, device_id_type=MESH)

        def tile_cols(n):
            return pl.ds(n * 256 if isinstance(n, int) else pl.multiple_of(n * 256, 256), 256)

        def put_stats(g, n, s1, s2):
            stat[g, me, 0:1, tile_cols(n)] = jnp.sum(s1, axis=0, keepdims=True)
            stat[g, me, 1:2, tile_cols(n)] = jnp.sum(s2, axis=0, keepdims=True)

        def fold(v):
            return jnp.sum(v.reshape(v.shape[0] // 8, 8, v.shape[1]), axis=0)

        lane = lax.broadcasted_iota(jnp.int32, (8, 128), 1)

        def group_totals(v):
            size = C // GROUPS
            parts = [v[:, i * 128:(i + 1) * 128] for i in range(C // 128)]
            done = [jnp.zeros((8, 128), F32) for _ in parts]
            for q in range(GROUPS):
                lo, hi = q * size, (q + 1) * size
                inside = [(i, (lane >= lo - i * 128) & (lane < hi - i * 128)) for i in range(lo // 128, (hi - 1) // 128 + 1)]
                picked = sum(jnp.where(m, parts[i], 0.0) for i, m in inside)
                total = jnp.sum(picked, axis=1, keepdims=True)
                for i, m in inside:
                    done[i] = jnp.where(m, total, done[i])
            return jnp.concatenate(done, axis=1)

        def exchange(g, then=None):
            for p in range(1, group_size):
                stat_copy(g, p).start()
            if then is not None:
                then()
            for p in range(1, group_size):
                stat_copy(g, p).wait_recv()
            total = stat[g, 0]
            for r in range(1, group_size):
                total = total + stat[g, r]
            for p in range(1, group_size):
                stat_copy(g, p).wait_send()
            s = group_totals(total)
            mean = s[0:1] / elem_count
            var = s[1:2] / elem_count - mean * mean
            norm[0:1] = mean
            norm[1:2] = lax.rsqrt(var + NORM_EPS) * norm_g[pl.ds(g, 1)]
            norm[2:3] = norm_b[pl.ds(g, 1)]

        def normed(v, k):
            cols = pl.ds(k * 256, 256)
            return (v.astype(F32) - norm[0:1, cols]) * norm[1:2, cols] + norm[2:3, cols]

        row_id = lax.broadcasted_iota(jnp.int32, (width, 256), 0)

        def activate(src, slot, f, k):
            for row in range(height):
                rows = slice(row * width, (row + 1) * width)
                z = normed(src[k, f * FR + row * width:f * FR + (row + 1) * width, :], k)
                z = z * lax.logistic(z)
                at = k * 3 * 256
                xs[slot][rows, at:at + 256] = jnp.where(row_id == 0, 0.0, pltpu.roll(z, 1, 0)).astype(BF)
                xs[slot][rows, at + 256:at + 512] = z.astype(BF)
                xs[slot][rows, at + 512:at + 768] = jnp.where(row_id == width - 1, 0.0, pltpu.roll(z, width - 1, 0)).astype(BF)

        def trip(slot, tap_t, n):
            for d in (1, 0, 2):
                w = jnp.concatenate([wbuf[slot, d, e, k * 256:(k + 1) * 256, :] for k in range(NT) for e in range(3)], axis=0)
                rows = FR if d == 1 else FR - width
                lo, dst = {0: (0, width), 1: (0, 0), 2: (width, 0)}[d]
                lhs = jnp.concatenate([xs[tap_t + f][lo:lo + rows, :] for f in range(2)], axis=0)
                r = jnp.dot(lhs, w, preferred_element_type=F32)
                if d == 1 and tap_t == 2:
                    acc[n] = r
                else:
                    for f in range(2):
                        acc[n, f * FR + dst:f * FR + dst + rows, :] += r[f * rows:(f + 1) * rows]

        def epilogue(c, n, g):
            odd = lax.rem(c, 2)
            bias = conv_b[pl.ds(c, 1), n * 256:(n + 1) * 256]
            keep = odd.astype(F32)
            s1 = jnp.zeros((8, 256), F32)
            s2 = jnp.zeros((8, 256), F32)
            for j in range(2 * height):
                rows = slice(j * width, (j + 1) * width)
                h = (acc[n, rows, :] + bias).astype(BF).astype(F32)
                h = (xres[n, rows, :].astype(F32) * keep + h).astype(BF)
                buf[1 - odd, n, rows, :] = h
                hf = h.astype(F32)
                s1 = s1 + fold(hf)
                s2 = s2 + fold(hf * hf)
            put_stats(g, n, s1, s2)

        def conv(c):
            base = c * units_conv
            g_in = c + c // 2
            src = buf.at[lax.rem(c, 2)]

            exchange(g_in, lambda: halo_start(c))

            for tap_t in (2, 1, 0):
                first = base + (2 - tap_t) * NT
                for n in range(NT):
                    for w in weight_copies(first + n):
                        w.wait()
                if tap_t < 2:
                    halo_wait(c, tap_t)
                if tap_t == 0:
                    halo_wait_send(c)

                @pl.when(me < group_size)
                def _():
                    if tap_t == 2:
                        for k in range(NT):
                            for f in range(2):
                                activate(src, 2 + f, f, k)
                    else:
                        for k in range(NT):
                            activate(halo.at[c], tap_t, tap_t, k)
                    for n in range(NT):
                        trip(lax.rem(first + n, RING), tap_t, n)
                        if tap_t == 0:
                            epilogue(c, n, g_in + 1)

                for n in range(NT):
                    @pl.when(first + n + RING < units_all)
                    def _():
                        for w in weight_copies(first + n + RING):
                            w.start()

        def attention(g):
            def rows_norm(j, carry):
                at = pl.ds(pl.multiple_of(j * width, width), width)
                for k in range(NT):
                    qkv[3, at, k * 256:(k + 1) * 256] = normed(xres[k, at, :], k).astype(BF)
                return carry

            lax.fori_loop(0, 2 * height, rows_norm, 0)
            attn_weight_copy().wait()
            for w in range(3):
                for n in range(NT):
                    cols = slice(n * 256, (n + 1) * 256)
                    v = jnp.dot(qkv[3], awbuf[w, :, cols], preferred_element_type=F32) + attn_b[w:w + 1, cols]
                    qkv[w, :, cols] = v.astype(BF)
            for f in range(2):
                rows = slice(f * FR, (f + 1) * FR)
                scores = lax.dot_general(qkv[0, rows, :], qkv[1, rows, :], (((1,), (1,)), ((), ())), preferred_element_type=F32)
                scores = scores * (C ** -0.5)
                e = jnp.exp(scores - jnp.max(scores, axis=1, keepdims=True))
                probs = (e / jnp.sum(e, axis=1, keepdims=True)).astype(BF)
                qkv[3, rows, :] = jnp.dot(probs, qkv[2, rows, :], preferred_element_type=F32).astype(BF)
            for n in range(NT):
                cols = slice(n * 256, (n + 1) * 256)
                h = (jnp.dot(qkv[3], awbuf[3, :, cols], preferred_element_type=F32) + attn_b[3:4, cols]).astype(BF)
                h = (xres[n].astype(F32) + h.astype(F32)).astype(BF)
                xres[n] = h
                hf = h.astype(F32)
                put_stats(g + 1, n, fold(hf), fold(hf * hf))

        for g in range(6):
            stat[g, me] = jnp.zeros((8, C), F32)
        for n in range(NT):
            in_copy(n).wait()
        pl.semaphore_wait(barrier, group_size - 1)
        for n in range(NT):
            def in_stats(j, carry):
                v = xres[n, pl.ds(pl.multiple_of(j * width, width), width), :].astype(F32)
                return carry[0] + fold(v), carry[1] + fold(v * v)

            s1, s2 = lax.fori_loop(0, 2 * height, in_stats, (jnp.zeros((8, 256), F32), jnp.zeros((8, 256), F32)))
            put_stats(0, n, s1, s2)
        def layer(c, carry):
            conv(c)

            @pl.when(c == 1)
            def _():
                exchange(2)
                attention(2)
            return carry

        lax.fori_loop(0, 4, layer, 0)
        for n in range(NT):
            out_copy(n).start()
        for n in range(NT):
            out_copy(n).wait()

    scratch = [
        pltpu.VMEM((RING, 3, 3, C, 256), BF),
        pltpu.VMEM((4, C, C), BF),
        pltpu.VMEM((FR, 3 * C), BF),
        pltpu.VMEM((FR, 3 * C), BF),
        pltpu.VMEM((FR, 3 * C), BF),
        pltpu.VMEM((FR, 3 * C), BF),
        pltpu.VMEM((2, NT, 2 * FR, 256), BF),
        pltpu.VMEM((4, NT, 2 * FR, 256), BF),
        pltpu.VMEM((NT, 2 * FR, 256), F32),
        pltpu.VMEM((4, 2 * FR, C), BF),
        pltpu.VMEM((6, group_size, 8, C), F32),
        pltpu.VMEM((8, C), F32),
        pltpu.SemaphoreType.DMA((RING, 3)),
        pltpu.SemaphoreType.DMA,
        pltpu.SemaphoreType.DMA((NT,)),
        pltpu.SemaphoreType.DMA((NT,)),
        pltpu.SemaphoreType.DMA((4, NT, 2)),
        pltpu.SemaphoreType.DMA((4, NT, 2)),
        pltpu.SemaphoreType.DMA((5, group_size)),
        pltpu.SemaphoreType.DMA((5, group_size)),
    ]
    return body, scratch


def solution(mesh):
    group_size = mesh.shape["time"]
    video_spec = P(("batch", "time"), None, None, None)

    def device_body(latent, conv_w, conv_b, norm_g, norm_b, attn_w, attn_b):
        frames, height, width, channels = latent.shape
        body, scratch = make_kernel(group_size, height, width, channels)
        hbm = pl.BlockSpec(memory_space=pltpu.HBM)
        vmem = pl.BlockSpec(memory_space=pltpu.VMEM)
        out = pl.pallas_call(
            body,
            out_shape=jax.ShapeDtypeStruct((frames * height * width, channels), BF),
            in_specs=[hbm, hbm, vmem, vmem, vmem, hbm, vmem],
            out_specs=hbm,
            scratch_shapes=scratch,
            compiler_params=pltpu.CompilerParams(collective_id=0, has_side_effects=True, vmem_limit_bytes=60 * 1024 * 1024),
            name="mid_block",
        )(latent.reshape(frames * height * width, channels), conv_w, conv_b, norm_g, norm_b, attn_w, attn_b)
        return out.reshape(latent.shape)

    return jax.shard_map(device_body, mesh=mesh, in_specs=(video_spec, P(), P(), P(), P(), P(), P()), out_specs=video_spec, check_vma=False)
```

```python
import jax
import jax.numpy as jnp
from jax import lax
from jax.experimental import pallas as pl
from jax.experimental.pallas import tpu as pltpu
from jax.sharding import PartitionSpec as P

GROUPS = 32
NORM_EPS = 1e-6
MESH = pl.DeviceIdType.MESH
BF = jnp.bfloat16
F32 = jnp.float32
RING = 6


def make_kernel(group_size, height, width, channels):
    C = channels
    NT = C // 256
    FR = height * width
    assert height == 4
    elem_count = float(group_size * 2 * FR * (C // GROUPS))
    units_conv = 3 * NT
    units_all = 4 * units_conv

    def body(latent, conv_w, conv_b, norm_g, norm_b, attn_w, attn_b, out,
             wbuf, awbuf, xs0, xs1, xs2, xs3, buf, halo, acc, qkv, stat, norm,
             wsem, awsem, insem, outsem, hsend, hrecv, ssend, srecv):
        me = lax.axis_index("time")
        xs = (xs0, xs1, xs2, xs3)
        xres = buf.at[0]

        def weight_copies(u):
            conv = u // units_conv
            rest = lax.rem(u, units_conv)
            tap_t = 2 - rest // NT
            tile = lax.rem(rest, NT)
            slot = lax.rem(u, RING)
            return [pltpu.make_async_copy(
                conv_w.at[conv, tap_t, d, :, :, pl.ds(pl.multiple_of(tile * 256, 256), 256)],
                wbuf.at[slot, d], wsem.at[slot, d]) for d in range(3)]

        def attn_weight_copy():
            return pltpu.make_async_copy(attn_w, awbuf, awsem)

        def in_copy(n):
            return pltpu.make_async_copy(latent.at[:, pl.ds(n * 256, 256)], xres.at[n], insem.at[n])

        def out_copy(n):
            return pltpu.make_async_copy(xres.at[n], out.at[:, pl.ds(n * 256, 256)], outsem.at[n])

        def halo_copy(conv, n, f):
            return pltpu.make_async_remote_copy(
                src_ref=buf.at[lax.rem(conv, 2), n, pl.ds(f * FR, FR)],
                dst_ref=halo.at[conv, n, pl.ds(f * FR, FR)],
                send_sem=hsend.at[conv, n, f], recv_sem=hrecv.at[conv, n, f],
                device_id={"time": lax.rem(me + 1, group_size)}, device_id_type=MESH)

        def first_copy(conv, n, f):
            return pltpu.make_async_copy(
                buf.at[lax.rem(conv, 2), n, pl.ds(0, FR)], halo.at[conv, n, pl.ds(f * FR, FR)], hrecv.at[conv, n, f])

        def halo_start(conv):
            @pl.when(me < group_size - 1)
            def _():
                for f in (1, 0):
                    for n in range(NT):
                        halo_copy(conv, n, f).start()

            @pl.when(me == 0)
            def _():
                for f in (1, 0):
                    for n in range(NT):
                        first_copy(conv, n, f).start()

        def halo_wait(conv, f):
            @pl.when(me == 0)
            def _():
                for n in range(NT):
                    first_copy(conv, n, f).wait()

            @pl.when(me > 0)
            def _():
                for n in range(NT):
                    halo_copy(conv, n, f).wait_recv()

        def halo_wait_send(conv):
            @pl.when(me < group_size - 1)
            def _():
                for n in range(NT):
                    for f in (1, 0):
                        halo_copy(conv, n, f).wait_send()

        def stat_copy(g, p):
            return pltpu.make_async_remote_copy(
                src_ref=stat.at[g, me], dst_ref=stat.at[g, me],
                send_sem=ssend.at[g, p], recv_sem=srecv.at[g, p],
                device_id={"time": lax.rem(me + p, group_size)}, device_id_type=MESH)

        def weights_start(lo, hi):
            for u in range(lo, hi):
                for w in weight_copies(u):
                    w.start()

        for n in range(NT):
            in_copy(n).start()

        barrier = pltpu.get_barrier_semaphore()
        for p in range(1, group_size):
            pl.semaphore_signal(barrier, inc=1, device_id={"time": lax.rem(me + p, group_size)}, device_id_type=MESH)

        def tile_cols(n):
            return pl.ds(n * 256 if isinstance(n, int) else pl.multiple_of(n * 256, 256), 256)

        def put_stats(g, n, s1, s2):
            stat[g, me, 0:1, tile_cols(n)] = jnp.sum(s1, axis=0, keepdims=True)
            stat[g, me, 1:2, tile_cols(n)] = jnp.sum(s2, axis=0, keepdims=True)

        def fold(v):
            return jnp.sum(v.reshape(v.shape[0] // 8, 8, v.shape[1]), axis=0)

        lane = lax.broadcasted_iota(jnp.int32, (2, 128), 1)

        def group_totals(v):
            size = C // GROUPS
            parts = [v[:, i * 128:(i + 1) * 128] for i in range(C // 128)]
            done = [jnp.zeros((2, 128), F32) for _ in parts]
            for q in range(GROUPS):
                lo, hi = q * size, (q + 1) * size
                inside = [(i, (lane >= lo - i * 128) & (lane < hi - i * 128)) for i in range(lo // 128, (hi - 1) // 128 + 1)]
                picked = sum(jnp.where(m, parts[i], 0.0) for i, m in inside)
                total = jnp.sum(picked, axis=1, keepdims=True)
                for i, m in inside:
                    done[i] = jnp.where(m, total, done[i])
            return jnp.concatenate(done, axis=1)

        def exchange(g, then=None):
            for p in range(1, group_size):
                stat_copy(g, p).start()
            if then is not None:
                then()
            for p in range(1, group_size):
                stat_copy(g, p).wait_recv()
            total = stat[g, 0]
            for r in range(1, group_size):
                total = total + stat[g, r]
            for p in range(1, group_size):
                stat_copy(g, p).wait_send()
            s = group_totals(total)
            mean = s[0:1] / elem_count
            var = s[1:2] / elem_count - mean * mean
            norm[0:1] = mean
            norm[1:2] = lax.rsqrt(var + NORM_EPS) * norm_g[pl.ds(g, 1)]
            norm[2:3] = norm_b[pl.ds(g, 1)]

        def normed(v, k):
            cols = pl.ds(k * 256, 256)
            return (v.astype(F32) - norm[0:1, cols]) * norm[1:2, cols] + norm[2:3, cols]

        row_id = lax.broadcasted_iota(jnp.int32, (width, 256), 0)

        def activate(src, slot, f, k):
            for row in range(height):
                rows = slice(row * width, (row + 1) * width)
                z = normed(src[k, f * FR + row * width:f * FR + (row + 1) * width, :], k)
                z = z * lax.logistic(z)
                at = k * 3 * 256
                xs[slot][rows, at:at + 256] = jnp.where(row_id == 0, 0.0, pltpu.roll(z, 1, 0)).astype(BF)
                xs[slot][rows, at + 256:at + 512] = z.astype(BF)
                xs[slot][rows, at + 512:at + 768] = jnp.where(row_id == width - 1, 0.0, pltpu.roll(z, width - 1, 0)).astype(BF)

        def trip(slot, tap_t, n):
            for d in (1, 0, 2):
                w = jnp.concatenate([wbuf[slot, d, e, k * 256:(k + 1) * 256, :] for k in range(NT) for e in range(3)], axis=0)
                rows = FR if d == 1 else FR - width
                lo, dst = {0: (0, width), 1: (0, 0), 2: (width, 0)}[d]
                lhs = jnp.concatenate([xs[tap_t + f][lo:lo + rows, :] for f in range(2)], axis=0)
                r = jnp.dot(lhs, w, preferred_element_type=F32)
                if d == 1 and tap_t == 2:
                    acc[n] = r
                else:
                    for f in range(2):
                        acc[n, f * FR + dst:f * FR + dst + rows, :] += r[f * rows:(f + 1) * rows]

        def epilogue(c, n, g):
            odd = lax.rem(c, 2)
            bias = conv_b[pl.ds(c, 1), n * 256:(n + 1) * 256]
            keep = odd.astype(F32)
            s1 = jnp.zeros((8, 256), F32)
            s2 = jnp.zeros((8, 256), F32)
            for j in range(2 * height):
                rows = slice(j * width, (j + 1) * width)
                h = (acc[n, rows, :] + bias).astype(BF).astype(F32)
                h = (xres[n, rows, :].astype(F32) * keep + h).astype(BF)
                buf[1 - odd, n, rows, :] = h
                hf = h.astype(F32)
                s1 = s1 + fold(hf)
                s2 = s2 + fold(hf * hf)
            put_stats(g, n, s1, s2)

        def conv(c):
            base = c * units_conv
            g_in = c + c // 2
            src = buf.at[lax.rem(c, 2)]

            exchange(g_in, lambda: halo_start(c))

            @pl.when(c == 0)
            def _():
                weights_start(NT, RING)

            for tap_t in (2, 1, 0):
                first = base + (2 - tap_t) * NT
                for n in range(NT):
                    for w in weight_copies(first + n):
                        w.wait()
                if tap_t < 2:
                    halo_wait(c, tap_t)
                if tap_t == 0:
                    halo_wait_send(c)

                @pl.when(me < group_size)
                def _():
                    if tap_t == 2:
                        for k in range(NT):
                            for f in range(2):
                                activate(src, 2 + f, f, k)
                    else:
                        for k in range(NT):
                            activate(halo.at[c], tap_t, tap_t, k)
                    for n in range(NT):
                        trip(lax.rem(first + n, RING), tap_t, n)
                        if tap_t == 0:
                            epilogue(c, n, g_in + 1)

                if tap_t == 1:
                    @pl.when(c == 0)
                    def _():
                        attn_weight_copy().start()
                for n in range(NT):
                    @pl.when(first + n + RING < units_all)
                    def _():
                        for w in weight_copies(first + n + RING):
                            w.start()

        def attention(g):
            def rows_norm(j, carry):
                at = pl.ds(pl.multiple_of(j * width, width), width)
                for k in range(NT):
                    qkv[3, at, k * 256:(k + 1) * 256] = normed(xres[k, at, :], k).astype(BF)
                return carry

            lax.fori_loop(0, 2 * height, rows_norm, 0)
            attn_weight_copy().wait()
            for w in range(3):
                for n in range(NT):
                    cols = slice(n * 256, (n + 1) * 256)
                    v = jnp.dot(qkv[3], awbuf[w, :, cols], preferred_element_type=F32) + attn_b[w:w + 1, cols]
                    qkv[w, :, cols] = v.astype(BF)
            for f in range(2):
                rows = slice(f * FR, (f + 1) * FR)
                scores = lax.dot_general(qkv[0, rows, :], qkv[1, rows, :], (((1,), (1,)), ((), ())), preferred_element_type=F32)
                scores = scores * (C ** -0.5)
                e = jnp.exp(scores - jnp.max(scores, axis=1, keepdims=True))
                probs = (e / jnp.sum(e, axis=1, keepdims=True)).astype(BF)
                qkv[3, rows, :] = jnp.dot(probs, qkv[2, rows, :], preferred_element_type=F32).astype(BF)
            for n in range(NT):
                cols = slice(n * 256, (n + 1) * 256)
                h = (jnp.dot(qkv[3], awbuf[3, :, cols], preferred_element_type=F32) + attn_b[3:4, cols]).astype(BF)
                h = (xres[n].astype(F32) + h.astype(F32)).astype(BF)
                xres[n] = h
                hf = h.astype(F32)
                put_stats(g + 1, n, fold(hf), fold(hf * hf))

        for n in range(NT):
            in_copy(n).wait()
        weights_start(0, NT)
        pl.semaphore_wait(barrier, group_size - 1)
        for n in range(NT):
            def in_stats(j, carry):
                v = xres[n, pl.ds(pl.multiple_of(j * width, width), width), :].astype(F32)
                return carry[0] + fold(v), carry[1] + fold(v * v)

            s1, s2 = lax.fori_loop(0, 2 * height, in_stats, (jnp.zeros((8, 256), F32), jnp.zeros((8, 256), F32)))
            put_stats(0, n, s1, s2)
        def layer(c, carry):
            conv(c)

            @pl.when(c == 1)
            def _():
                exchange(2)
                attention(2)
            return carry

        lax.fori_loop(0, 4, layer, 0)
        for n in range(NT):
            out_copy(n).start()
        for n in range(NT):
            out_copy(n).wait()

    scratch = [
        pltpu.VMEM((RING, 3, 3, C, 256), BF),
        pltpu.VMEM((4, C, C), BF),
        pltpu.VMEM((FR, 3 * C), BF),
        pltpu.VMEM((FR, 3 * C), BF),
        pltpu.VMEM((FR, 3 * C), BF),
        pltpu.VMEM((FR, 3 * C), BF),
        pltpu.VMEM((2, NT, 2 * FR, 256), BF),
        pltpu.VMEM((4, NT, 2 * FR, 256), BF),
        pltpu.VMEM((NT, 2 * FR, 256), F32),
        pltpu.VMEM((4, 2 * FR, C), BF),
        pltpu.VMEM((6, group_size, 2, C), F32),
        pltpu.VMEM((8, C), F32),
        pltpu.SemaphoreType.DMA((RING, 3)),
        pltpu.SemaphoreType.DMA,
        pltpu.SemaphoreType.DMA((NT,)),
        pltpu.SemaphoreType.DMA((NT,)),
        pltpu.SemaphoreType.DMA((4, NT, 2)),
        pltpu.SemaphoreType.DMA((4, NT, 2)),
        pltpu.SemaphoreType.DMA((5, group_size)),
        pltpu.SemaphoreType.DMA((5, group_size)),
    ]
    return body, scratch


def solution(mesh):
    group_size = mesh.shape["time"]
    video_spec = P(("batch", "time"), None, None, None)

    def device_body(latent, conv_w, conv_b, norm_g, norm_b, attn_w, attn_b):
        frames, height, width, channels = latent.shape
        body, scratch = make_kernel(group_size, height, width, channels)
        hbm = pl.BlockSpec(memory_space=pltpu.HBM)
        vmem = pl.BlockSpec(memory_space=pltpu.VMEM)
        out = pl.pallas_call(
            body,
            out_shape=jax.ShapeDtypeStruct((frames * height * width, channels), BF),
            in_specs=[hbm, hbm, vmem, vmem, vmem, hbm, vmem],
            out_specs=pl.BlockSpec(memory_space=pl.ANY),
            scratch_shapes=scratch,
            compiler_params=pltpu.CompilerParams(collective_id=0, has_side_effects=True, vmem_limit_bytes=52 * 1024 * 1024),
            name="mid_block",
        )(latent.reshape(frames * height * width, channels), conv_w, conv_b, norm_g, norm_b, attn_w, attn_b)
        return out.reshape(latent.shape)

    return jax.shard_map(device_body, mesh=mesh, in_specs=(video_spec, P(), P(), P(), P(), P(), P()), out_specs=video_spec, check_vma=False)
```

```python
import jax
import jax.numpy as jnp
from jax import lax
from jax.experimental import pallas as pl
from jax.experimental.pallas import tpu as pltpu
from jax.sharding import PartitionSpec as P

GROUPS = 32
NORM_EPS = 1e-6
MESH = pl.DeviceIdType.MESH
BF = jnp.bfloat16
F32 = jnp.float32
RING = 6


def make_kernel(group_size, height, width, channels):
    C = channels
    NT = C // 256
    FR = height * width
    assert height == 4
    elem_count = float(group_size * 2 * FR * (C // GROUPS))
    units_conv = 3 * NT
    units_all = 4 * units_conv

    def body(latent, conv_w, conv_b_in, norm_g_in, norm_b_in, attn_w, attn_b_in, out,
             conv_b, norm_g, norm_b, attn_b, wbuf, awbuf, xs0, xs1, xs2, xs3, buf, halo, acc, qkv, stat, norm,
             psem, wsem, awsem, insem, outsem, hsend, hrecv, ssend, srecv):
        me = lax.axis_index("time")
        xs = (xs0, xs1, xs2, xs3)
        xres = buf.at[0]

        def weight_copies(u):
            conv = u // units_conv
            rest = lax.rem(u, units_conv)
            tap_t = 2 - rest // NT
            tile = lax.rem(rest, NT)
            slot = lax.rem(u, RING)
            return [pltpu.make_async_copy(
                conv_w.at[conv, tap_t, d, :, :, pl.ds(pl.multiple_of(tile * 256, 256), 256)],
                wbuf.at[slot, d], wsem.at[slot, d]) for d in range(3)]

        def attn_weight_copy():
            return pltpu.make_async_copy(attn_w, awbuf, awsem)

        def in_copy(n):
            return pltpu.make_async_copy(latent.at[:, pl.ds(n * 256, 256)], xres.at[n], insem.at[n])

        def out_copy(n):
            return pltpu.make_async_copy(xres.at[n], out.at[:, pl.ds(n * 256, 256)], outsem.at[n])

        def halo_copy(conv, n, f):
            return pltpu.make_async_remote_copy(
                src_ref=buf.at[lax.rem(conv, 2), n, pl.ds(f * FR, FR)],
                dst_ref=halo.at[conv, n, pl.ds(f * FR, FR)],
                send_sem=hsend.at[conv, n, f], recv_sem=hrecv.at[conv, n, f],
                device_id={"time": lax.rem(me + 1, group_size)}, device_id_type=MESH)

        def first_copy(conv, n, f):
            return pltpu.make_async_copy(
                buf.at[lax.rem(conv, 2), n, pl.ds(0, FR)], halo.at[conv, n, pl.ds(f * FR, FR)], hrecv.at[conv, n, f])

        def halo_start(conv):
            @pl.when(me < group_size - 1)
            def _():
                for f in (1, 0):
                    for n in range(NT):
                        halo_copy(conv, n, f).start()

            @pl.when(me == 0)
            def _():
                for f in (1, 0):
                    for n in range(NT):
                        first_copy(conv, n, f).start()

        def halo_wait(conv, f):
            @pl.when(me == 0)
            def _():
                for n in range(NT):
                    first_copy(conv, n, f).wait()

            @pl.when(me > 0)
            def _():
                for n in range(NT):
                    halo_copy(conv, n, f).wait_recv()

        def halo_wait_send(conv):
            @pl.when(me < group_size - 1)
            def _():
                for n in range(NT):
                    for f in (1, 0):
                        halo_copy(conv, n, f).wait_send()

        def stat_copy(g, p):
            return pltpu.make_async_remote_copy(
                src_ref=stat.at[g, me], dst_ref=stat.at[g, me],
                send_sem=ssend.at[g, p], recv_sem=srecv.at[g, p],
                device_id={"time": lax.rem(me + p, group_size)}, device_id_type=MESH)

        def weights_start(lo, hi):
            for u in range(lo, hi):
                for w in weight_copies(u):
                    w.start()

        small = [pltpu.make_async_copy(a, b, psem.at[i]) for i, (a, b) in enumerate(
            ((conv_b_in, conv_b), (norm_g_in, norm_g), (norm_b_in, norm_b), (attn_b_in, attn_b)))]
        for n in range(NT):
            in_copy(n).start()
        for p in small:
            p.start()

        barrier = pltpu.get_barrier_semaphore()
        for p in range(1, group_size):
            pl.semaphore_signal(barrier, inc=1, device_id={"time": lax.rem(me + p, group_size)}, device_id_type=MESH)

        def tile_cols(n):
            return pl.ds(n * 256 if isinstance(n, int) else pl.multiple_of(n * 256, 256), 256)

        def put_stats(g, n, s1, s2):
            stat[g, me, 0:1, tile_cols(n)] = jnp.sum(s1, axis=0, keepdims=True)
            stat[g, me, 1:2, tile_cols(n)] = jnp.sum(s2, axis=0, keepdims=True)

        def fold(v):
            return jnp.sum(v.reshape(v.shape[0] // 8, 8, v.shape[1]), axis=0)

        lane = lax.broadcasted_iota(jnp.int32, (2, 128), 1)

        def group_totals(v):
            size = C // GROUPS
            parts = [v[:, i * 128:(i + 1) * 128] for i in range(C // 128)]
            done = [jnp.zeros((2, 128), F32) for _ in parts]
            for q in range(GROUPS):
                lo, hi = q * size, (q + 1) * size
                inside = [(i, (lane >= lo - i * 128) & (lane < hi - i * 128)) for i in range(lo // 128, (hi - 1) // 128 + 1)]
                picked = sum(jnp.where(m, parts[i], 0.0) for i, m in inside)
                total = jnp.sum(picked, axis=1, keepdims=True)
                for i, m in inside:
                    done[i] = jnp.where(m, total, done[i])
            return jnp.concatenate(done, axis=1)

        def exchange(g, then=None):
            for p in range(1, group_size):
                stat_copy(g, p).start()
            if then is not None:
                then()
            for p in range(1, group_size):
                stat_copy(g, p).wait_recv()
            total = stat[g, 0]
            for r in range(1, group_size):
                total = total + stat[g, r]
            for p in range(1, group_size):
                stat_copy(g, p).wait_send()
            s = group_totals(total)
            mean = s[0:1] / elem_count
            var = s[1:2] / elem_count - mean * mean
            norm[0:1] = mean
            norm[1:2] = lax.rsqrt(var + NORM_EPS) * norm_g[pl.ds(g, 1)]
            norm[2:3] = norm_b[pl.ds(g, 1)]

        def normed(v, k):
            cols = pl.ds(k * 256, 256)
            return (v.astype(F32) - norm[0:1, cols]) * norm[1:2, cols] + norm[2:3, cols]

        row_id = lax.broadcasted_iota(jnp.int32, (width, 256), 0)

        def activate(src, slot, f, k):
            for row in range(height):
                rows = slice(row * width, (row + 1) * width)
                z = normed(src[k, f * FR + row * width:f * FR + (row + 1) * width, :], k)
                z = z * lax.logistic(z)
                at = k * 3 * 256
                xs[slot][rows, at:at + 256] = jnp.where(row_id == 0, 0.0, pltpu.roll(z, 1, 0)).astype(BF)
                xs[slot][rows, at + 256:at + 512] = z.astype(BF)
                xs[slot][rows, at + 512:at + 768] = jnp.where(row_id == width - 1, 0.0, pltpu.roll(z, width - 1, 0)).astype(BF)

        def trip(slot, tap_t, n):
            for d in (1, 0, 2):
                w = jnp.concatenate([wbuf[slot, d, e, k * 256:(k + 1) * 256, :] for k in range(NT) for e in range(3)], axis=0)
                rows = FR if d == 1 else FR - width
                lo, dst = {0: (0, width), 1: (0, 0), 2: (width, 0)}[d]
                lhs = jnp.concatenate([xs[tap_t + f][lo:lo + rows, :] for f in range(2)], axis=0)
                r = jnp.dot(lhs, w, preferred_element_type=F32)
                if d == 1 and tap_t == 2:
                    acc[n] = r
                else:
                    for f in range(2):
                        acc[n, f * FR + dst:f * FR + dst + rows, :] += r[f * rows:(f + 1) * rows]

        def epilogue(c, n, g):
            odd = lax.rem(c, 2)
            bias = conv_b[pl.ds(c, 1), n * 256:(n + 1) * 256]
            keep = odd.astype(F32)
            s1 = jnp.zeros((8, 256), F32)
            s2 = jnp.zeros((8, 256), F32)
            for j in range(2 * height):
                rows = slice(j * width, (j + 1) * width)
                h = (acc[n, rows, :] + bias).astype(BF).astype(F32)
                h = (xres[n, rows, :].astype(F32) * keep + h).astype(BF)
                buf[1 - odd, n, rows, :] = h
                hf = h.astype(F32)
                s1 = s1 + fold(hf)
                s2 = s2 + fold(hf * hf)
            put_stats(g, n, s1, s2)

        def conv(c):
            base = c * units_conv
            g_in = c + c // 2
            src = buf.at[lax.rem(c, 2)]

            exchange(g_in, lambda: halo_start(c))

            @pl.when(c == 0)
            def _():
                weights_start(NT, RING)

            for tap_t in (2, 1, 0):
                first = base + (2 - tap_t) * NT
                for n in range(NT):
                    for w in weight_copies(first + n):
                        w.wait()
                if tap_t < 2:
                    halo_wait(c, tap_t)
                if tap_t == 0:
                    halo_wait_send(c)

                @pl.when(me < group_size)
                def _():
                    if tap_t == 2:
                        for k in range(NT):
                            for f in range(2):
                                activate(src, 2 + f, f, k)
                    else:
                        for k in range(NT):
                            activate(halo.at[c], tap_t, tap_t, k)
                    for n in range(NT):
                        trip(lax.rem(first + n, RING), tap_t, n)
                        if tap_t == 0:
                            epilogue(c, n, g_in + 1)

                if tap_t == 1:
                    @pl.when(c == 0)
                    def _():
                        attn_weight_copy().start()
                for n in range(NT):
                    @pl.when(first + n + RING < units_all)
                    def _():
                        for w in weight_copies(first + n + RING):
                            w.start()

        def attention(g):
            attn_weight_copy().wait()
            for k in range(NT):
                for j in range(2 * height):
                    at = slice(j * width, (j + 1) * width)
                    qkv[3, at, k * 256:(k + 1) * 256] = normed(xres[k, at, :], k).astype(BF)
            for w in range(3):
                for n in range(NT):
                    cols = slice(n * 256, (n + 1) * 256)
                    for f in range(2):
                        rows = slice(f * FR, (f + 1) * FR)
                        v = jnp.dot(qkv[3, rows, :], awbuf[w, :, cols], preferred_element_type=F32) + attn_b[w:w + 1, cols]
                        qkv[w, rows, cols] = v.astype(BF)
            for f in range(2):
                rows = slice(f * FR, (f + 1) * FR)
                scores = lax.dot_general(qkv[0, rows, :], qkv[1, rows, :], (((1,), (1,)), ((), ())), preferred_element_type=F32)
                scores = scores * (C ** -0.5)
                e = jnp.exp(scores - jnp.max(scores, axis=1, keepdims=True))
                probs = (e / jnp.sum(e, axis=1, keepdims=True)).astype(BF)
                qkv[3, rows, :] = jnp.dot(probs, qkv[2, rows, :], preferred_element_type=F32).astype(BF)
            for n in range(NT):
                cols = slice(n * 256, (n + 1) * 256)
                s1 = jnp.zeros((8, 256), F32)
                s2 = jnp.zeros((8, 256), F32)
                for f in range(2):
                    rows = slice(f * FR, (f + 1) * FR)
                    h = (jnp.dot(qkv[3, rows, :], awbuf[3, :, cols], preferred_element_type=F32) + attn_b[3:4, cols]).astype(BF)
                    h = (xres[n, rows, :].astype(F32) + h.astype(F32)).astype(BF)
                    xres[n, rows, :] = h
                    hf = h.astype(F32)
                    s1 = s1 + fold(hf)
                    s2 = s2 + fold(hf * hf)
                put_stats(g + 1, n, s1, s2)

        for n in range(NT):
            in_copy(n).wait()
        weights_start(0, NT)
        for p in small:
            p.wait()
        pl.semaphore_wait(barrier, group_size - 1)
        for n in range(NT):
            def in_stats(j, carry):
                v = xres[n, pl.ds(pl.multiple_of(j * width, width), width), :].astype(F32)
                return carry[0] + fold(v), carry[1] + fold(v * v)

            s1, s2 = lax.fori_loop(0, 2 * height, in_stats, (jnp.zeros((8, 256), F32), jnp.zeros((8, 256), F32)))
            put_stats(0, n, s1, s2)
        def layer(c, carry):
            conv(c)

            @pl.when(c == 1)
            def _():
                exchange(2)
                attention(2)
            return carry

        lax.fori_loop(0, 4, layer, 0)
        for n in range(NT):
            out_copy(n).start()
        for n in range(NT):
            out_copy(n).wait()

    scratch = [
        pltpu.VMEM((4, C), F32),
        pltpu.VMEM((5, C), F32),
        pltpu.VMEM((5, C), F32),
        pltpu.VMEM((4, C), F32),
        pltpu.VMEM((RING, 3, 3, C, 256), BF),
        pltpu.VMEM((4, C, C), BF),
        pltpu.VMEM((FR, 3 * C), BF),
        pltpu.VMEM((FR, 3 * C), BF),
        pltpu.VMEM((FR, 3 * C), BF),
        pltpu.VMEM((FR, 3 * C), BF),
        pltpu.VMEM((2, NT, 2 * FR, 256), BF),
        pltpu.VMEM((4, NT, 2 * FR, 256), BF),
        pltpu.VMEM((NT, 2 * FR, 256), F32),
        pltpu.VMEM((4, 2 * FR, C), BF),
        pltpu.VMEM((6, group_size, 2, C), F32),
        pltpu.VMEM((8, C), F32),
        pltpu.SemaphoreType.DMA((4,)),
        pltpu.SemaphoreType.DMA((RING, 3)),
        pltpu.SemaphoreType.DMA,
        pltpu.SemaphoreType.DMA((NT,)),
        pltpu.SemaphoreType.DMA((NT,)),
        pltpu.SemaphoreType.DMA((4, NT, 2)),
        pltpu.SemaphoreType.DMA((4, NT, 2)),
        pltpu.SemaphoreType.DMA((5, group_size)),
        pltpu.SemaphoreType.DMA((5, group_size)),
    ]
    return body, scratch


def solution(mesh):
    group_size = mesh.shape["time"]
    video_spec = P(("batch", "time"), None, None, None)

    def device_body(latent, conv_w, conv_b, norm_g, norm_b, attn_w, attn_b):
        frames, height, width, channels = latent.shape
        body, scratch = make_kernel(group_size, height, width, channels)
        pinned = [pltpu.with_memory_space_constraint(p, pltpu.HBM) for p in (conv_b, norm_g, norm_b, attn_b)]
        hbm = pl.BlockSpec(memory_space=pltpu.HBM)
        out = pl.pallas_call(
            body,
            out_shape=jax.ShapeDtypeStruct((frames * height * width, channels), BF),
            in_specs=[hbm] * 7,
            out_specs=pl.BlockSpec(memory_space=pl.ANY),
            scratch_shapes=scratch,
            compiler_params=pltpu.CompilerParams(collective_id=0, has_side_effects=True, vmem_limit_bytes=52 * 1024 * 1024),
            name="mid_block",
        )(latent.reshape(frames * height * width, channels), conv_w, *pinned[:3], attn_w, pinned[3])
        return out.reshape(latent.shape)

    return jax.shard_map(device_body, mesh=mesh, in_specs=(video_spec, P(), P(), P(), P(), P(), P()), out_specs=video_spec, check_vma=False)
```

```python
import jax
import jax.numpy as jnp
from jax import lax
from jax.experimental import pallas as pl
from jax.experimental.pallas import tpu as pltpu
from jax.sharding import PartitionSpec as P

GROUPS = 32
NORM_EPS = 1e-6
MESH = pl.DeviceIdType.MESH
BF = jnp.bfloat16
F32 = jnp.float32
RING = 6


def make_kernel(group_size, height, width, channels):
    C = channels
    NT = C // 256
    FR = height * width
    assert height == 4
    elem_count = float(group_size * 2 * FR * (C // GROUPS))
    units_conv = 3 * NT
    units_all = 4 * units_conv

    def body(latent, conv_w, conv_b_in, norm_g_in, norm_b_in, attn_w, attn_b_in, out,
             conv_b, norm_g, norm_b, attn_b, wbuf, awbuf, xs0, xs1, xs2, xs3, buf, halo, acc, qkv, stat, norm,
             psem, wsem, awsem, insem, hsend, hrecv, ssend, srecv):
        me = lax.axis_index("time")
        xs = (xs0, xs1, xs2, xs3)
        xres = buf.at[0]

        def weight_copies(u):
            conv = u // units_conv
            rest = lax.rem(u, units_conv)
            tap_t = 2 - rest // NT
            tile = lax.rem(rest, NT)
            slot = lax.rem(u, RING)
            return [pltpu.make_async_copy(
                conv_w.at[conv, tap_t, d, :, :, pl.ds(pl.multiple_of(tile * 256, 256), 256)],
                wbuf.at[slot, d], wsem.at[slot, d]) for d in range(3)]

        def attn_weight_copy():
            return pltpu.make_async_copy(attn_w, awbuf, awsem)

        def in_copy(n):
            return pltpu.make_async_copy(latent.at[:, pl.ds(n * 256, 256)], xres.at[n], insem.at[n])

        def halo_copy(conv, n, f):
            return pltpu.make_async_remote_copy(
                src_ref=buf.at[lax.rem(conv, 2), n, pl.ds(f * FR, FR)],
                dst_ref=halo.at[conv, n, pl.ds(f * FR, FR)],
                send_sem=hsend.at[conv, n, f], recv_sem=hrecv.at[conv, n, f],
                device_id={"time": lax.rem(me + 1, group_size)}, device_id_type=MESH)

        def first_copy(conv, n, f):
            return pltpu.make_async_copy(
                buf.at[lax.rem(conv, 2), n, pl.ds(0, FR)], halo.at[conv, n, pl.ds(f * FR, FR)], hrecv.at[conv, n, f])

        def halo_start(conv):
            @pl.when(me < group_size - 1)
            def _():
                for f in (1, 0):
                    for n in range(NT):
                        halo_copy(conv, n, f).start()

            @pl.when(me == 0)
            def _():
                for f in (1, 0):
                    for n in range(NT):
                        first_copy(conv, n, f).start()

        def halo_wait(conv, f):
            @pl.when(me == 0)
            def _():
                for n in range(NT):
                    first_copy(conv, n, f).wait()

            @pl.when(me > 0)
            def _():
                for n in range(NT):
                    halo_copy(conv, n, f).wait_recv()

        def halo_wait_send(conv):
            @pl.when(me < group_size - 1)
            def _():
                for n in range(NT):
                    for f in (1, 0):
                        halo_copy(conv, n, f).wait_send()

        def stat_copy(g, p):
            return pltpu.make_async_remote_copy(
                src_ref=stat.at[g, me], dst_ref=stat.at[g, me],
                send_sem=ssend.at[g, p], recv_sem=srecv.at[g, p],
                device_id={"time": lax.rem(me + p, group_size)}, device_id_type=MESH)

        def weights_start(lo, hi):
            for u in range(lo, hi):
                for w in weight_copies(u):
                    w.start()

        small = [pltpu.make_async_copy(a, b, psem.at[i]) for i, (a, b) in enumerate(
            ((conv_b_in, conv_b), (norm_g_in, norm_g), (norm_b_in, norm_b), (attn_b_in, attn_b)))]
        for n in range(NT):
            in_copy(n).start()
        for p in small:
            p.start()

        barrier = pltpu.get_barrier_semaphore()
        for p in range(1, group_size):
            pl.semaphore_signal(barrier, inc=1, device_id={"time": lax.rem(me + p, group_size)}, device_id_type=MESH)

        def tile_cols(n):
            return pl.ds(n * 256 if isinstance(n, int) else pl.multiple_of(n * 256, 256), 256)

        def put_stats(g, n, s1, s2):
            stat[g, me, 0:1, tile_cols(n)] = jnp.sum(s1, axis=0, keepdims=True)
            stat[g, me, 1:2, tile_cols(n)] = jnp.sum(s2, axis=0, keepdims=True)

        def fold(v):
            return jnp.sum(v.reshape(v.shape[0] // 8, 8, v.shape[1]), axis=0)

        lane = lax.broadcasted_iota(jnp.int32, (2, 128), 1)

        def group_totals(v):
            size = C // GROUPS
            parts = [v[:, i * 128:(i + 1) * 128] for i in range(C // 128)]
            done = [jnp.zeros((2, 128), F32) for _ in parts]
            for q in range(GROUPS):
                lo, hi = q * size, (q + 1) * size
                inside = [(i, (lane >= lo - i * 128) & (lane < hi - i * 128)) for i in range(lo // 128, (hi - 1) // 128 + 1)]
                picked = sum(jnp.where(m, parts[i], 0.0) for i, m in inside)
                total = jnp.sum(picked, axis=1, keepdims=True)
                for i, m in inside:
                    done[i] = jnp.where(m, total, done[i])
            return jnp.concatenate(done, axis=1)

        def exchange(g, then=None):
            for p in range(1, group_size):
                stat_copy(g, p).start()
            if then is not None:
                then()
            for p in range(1, group_size):
                stat_copy(g, p).wait_recv()
            total = stat[g, 0]
            for r in range(1, group_size):
                total = total + stat[g, r]
            for p in range(1, group_size):
                stat_copy(g, p).wait_send()
            s = group_totals(total)
            mean = s[0:1] / elem_count
            var = s[1:2] / elem_count - mean * mean
            norm[0:1] = mean
            norm[1:2] = lax.rsqrt(var + NORM_EPS) * norm_g[pl.ds(g, 1)]
            norm[2:3] = norm_b[pl.ds(g, 1)]

        def normed(v, k):
            cols = pl.ds(k * 256, 256)
            return (v.astype(F32) - norm[0:1, cols]) * norm[1:2, cols] + norm[2:3, cols]

        row_id = lax.broadcasted_iota(jnp.int32, (width, 256), 0)

        def activate(src, slot, f, k):
            for row in range(height):
                rows = slice(row * width, (row + 1) * width)
                z = normed(src[k, f * FR + row * width:f * FR + (row + 1) * width, :], k)
                z = z * lax.logistic(z)
                at = k * 3 * 256
                xs[slot][rows, at:at + 256] = jnp.where(row_id == 0, 0.0, pltpu.roll(z, 1, 0)).astype(BF)
                xs[slot][rows, at + 256:at + 512] = z.astype(BF)
                xs[slot][rows, at + 512:at + 768] = jnp.where(row_id == width - 1, 0.0, pltpu.roll(z, width - 1, 0)).astype(BF)

        def trip(slot, tap_t, n):
            for d in ((1, 0, 2) if tap_t == 2 else (0, 2, 1)):
                w = jnp.concatenate([wbuf[slot, d, e, k * 256:(k + 1) * 256, :] for k in range(NT) for e in range(3)], axis=0)
                rows = FR if d == 1 else FR - width
                lo, dst = {0: (0, width), 1: (0, 0), 2: (width, 0)}[d]
                order = (0, 1) if tap_t == 2 else (1, 0)
                lhs = jnp.concatenate([xs[tap_t + f][lo:lo + rows, :] for f in order], axis=0)
                r = jnp.dot(lhs, w, preferred_element_type=F32)
                if d == 1 and tap_t == 2:
                    acc[n] = r
                else:
                    for at, f in enumerate(order):
                        acc[n, f * FR + dst:f * FR + dst + rows, :] += r[at * rows:(at + 1) * rows]

        def epilogue(c, n, g):
            odd = lax.rem(c, 2)
            bias = conv_b[pl.ds(c, 1), n * 256:(n + 1) * 256]
            keep = odd.astype(F32)
            s1 = jnp.zeros((8, 256), F32)
            s2 = jnp.zeros((8, 256), F32)
            for j in range(2 * height):
                rows = slice(j * width, (j + 1) * width)
                h = (acc[n, rows, :] + bias).astype(BF).astype(F32)
                h = (xres[n, rows, :].astype(F32) * keep + h).astype(BF)
                buf[1 - odd, n, rows, :] = h
                out[rows, n * 256:(n + 1) * 256] = h
                hf = h.astype(F32)
                s1 = s1 + fold(hf)
                s2 = s2 + fold(hf * hf)
            put_stats(g, n, s1, s2)

        def conv(c):
            base = c * units_conv
            g_in = c + c // 2
            src = buf.at[lax.rem(c, 2)]

            exchange(g_in, lambda: halo_start(c))

            @pl.when(c == 0)
            def _():
                weights_start(NT, RING)

            for tap_t in (2, 1, 0):
                first = base + (2 - tap_t) * NT
                for n in range(NT):
                    for w in weight_copies(first + n):
                        w.wait()
                if tap_t < 2:
                    halo_wait(c, tap_t)
                if tap_t == 0:
                    halo_wait_send(c)

                @pl.when(me < group_size)
                def _():
                    if tap_t == 2:
                        for k in range(NT):
                            for f in range(2):
                                activate(src, 2 + f, f, k)
                    else:
                        for k in range(NT):
                            activate(halo.at[c], tap_t, tap_t, k)
                    for n in range(NT):
                        trip(lax.rem(first + n, RING), tap_t, n)
                        if tap_t == 0:
                            epilogue(c, n, g_in + 1)

                if tap_t == 1:
                    @pl.when(c == 0)
                    def _():
                        attn_weight_copy().start()
                for n in range(NT):
                    @pl.when(first + n + RING < units_all)
                    def _():
                        for w in weight_copies(first + n + RING):
                            w.start()

        def attention(g):
            attn_weight_copy().wait()
            for k in range(NT):
                for j in range(2 * height):
                    at = slice(j * width, (j + 1) * width)
                    qkv[3, at, k * 256:(k + 1) * 256] = normed(xres[k, at, :], k).astype(BF)
            for w in range(3):
                for n in range(NT):
                    cols = slice(n * 256, (n + 1) * 256)
                    for f in range(2):
                        rows = slice(f * FR, (f + 1) * FR)
                        v = jnp.dot(qkv[3, rows, :], awbuf[w, :, cols], preferred_element_type=F32) + attn_b[w:w + 1, cols]
                        qkv[w, rows, cols] = v.astype(BF)
            for f in range(2):
                rows = slice(f * FR, (f + 1) * FR)
                scores = lax.dot_general(qkv[0, rows, :], qkv[1, rows, :], (((1,), (1,)), ((), ())), preferred_element_type=F32)
                scores = scores * (C ** -0.5)
                e = jnp.exp(scores - jnp.max(scores, axis=1, keepdims=True))
                probs = (e / jnp.sum(e, axis=1, keepdims=True)).astype(BF)
                qkv[3, rows, :] = jnp.dot(probs, qkv[2, rows, :], preferred_element_type=F32).astype(BF)
            for n in range(NT):
                cols = slice(n * 256, (n + 1) * 256)
                s1 = jnp.zeros((8, 256), F32)
                s2 = jnp.zeros((8, 256), F32)
                for f in range(2):
                    rows = slice(f * FR, (f + 1) * FR)
                    h = (jnp.dot(qkv[3, rows, :], awbuf[3, :, cols], preferred_element_type=F32) + attn_b[3:4, cols]).astype(BF)
                    h = (xres[n, rows, :].astype(F32) + h.astype(F32)).astype(BF)
                    xres[n, rows, :] = h
                    hf = h.astype(F32)
                    s1 = s1 + fold(hf)
                    s2 = s2 + fold(hf * hf)
                put_stats(g + 1, n, s1, s2)

        for n in range(NT):
            in_copy(n).wait()
        weights_start(0, NT)
        for p in small:
            p.wait()
        pl.semaphore_wait(barrier, group_size - 1)
        for n in range(NT):
            def in_stats(j, carry):
                v = xres[n, pl.ds(pl.multiple_of(j * width, width), width), :].astype(F32)
                return carry[0] + fold(v), carry[1] + fold(v * v)

            s1, s2 = lax.fori_loop(0, 2 * height, in_stats, (jnp.zeros((8, 256), F32), jnp.zeros((8, 256), F32)))
            put_stats(0, n, s1, s2)
        def layer(c, carry):
            conv(c)

            @pl.when(c == 1)
            def _():
                exchange(2)
                attention(2)
            return carry

        lax.fori_loop(0, 4, layer, 0)

    scratch = [
        pltpu.VMEM((4, C), F32),
        pltpu.VMEM((5, C), F32),
        pltpu.VMEM((5, C), F32),
        pltpu.VMEM((4, C), F32),
        pltpu.VMEM((RING, 3, 3, C, 256), BF),
        pltpu.VMEM((4, C, C), BF),
        pltpu.VMEM((FR, 3 * C), BF),
        pltpu.VMEM((FR, 3 * C), BF),
        pltpu.VMEM((FR, 3 * C), BF),
        pltpu.VMEM((FR, 3 * C), BF),
        pltpu.VMEM((2, NT, 2 * FR, 256), BF),
        pltpu.VMEM((4, NT, 2 * FR, 256), BF),
        pltpu.VMEM((NT, 2 * FR, 256), F32),
        pltpu.VMEM((4, 2 * FR, C), BF),
        pltpu.VMEM((6, group_size, 2, C), F32),
        pltpu.VMEM((8, C), F32),
        pltpu.SemaphoreType.DMA((4,)),
        pltpu.SemaphoreType.DMA((RING, 3)),
        pltpu.SemaphoreType.DMA,
        pltpu.SemaphoreType.DMA((NT,)),
        pltpu.SemaphoreType.DMA((4, NT, 2)),
        pltpu.SemaphoreType.DMA((4, NT, 2)),
        pltpu.SemaphoreType.DMA((5, group_size)),
        pltpu.SemaphoreType.DMA((5, group_size)),
    ]
    return body, scratch


def solution(mesh):
    group_size = mesh.shape["time"]
    video_spec = P(("batch", "time"), None, None, None)

    def device_body(latent, conv_w, conv_b, norm_g, norm_b, attn_w, attn_b):
        frames, height, width, channels = latent.shape
        body, scratch = make_kernel(group_size, height, width, channels)
        pinned = [pltpu.with_memory_space_constraint(p, pltpu.HBM) for p in (conv_b, norm_g, norm_b, attn_b)]
        hbm = pl.BlockSpec(memory_space=pltpu.HBM)
        out = pl.pallas_call(
            body,
            out_shape=jax.ShapeDtypeStruct((frames * height * width, channels), BF),
            in_specs=[hbm] * 7,
            out_specs=pl.BlockSpec(memory_space=pltpu.VMEM),
            scratch_shapes=scratch,
            compiler_params=pltpu.CompilerParams(collective_id=0, has_side_effects=True, vmem_limit_bytes=52 * 1024 * 1024),
            name="mid_block",
        )(latent.reshape(frames * height * width, channels), conv_w, *pinned[:3], attn_w, pinned[3])
        return out.reshape(latent.shape)

    return jax.shard_map(device_body, mesh=mesh, in_specs=(video_spec, P(), P(), P(), P(), P(), P()), out_specs=video_spec, check_vma=False)
```

```python
import jax
import jax.numpy as jnp
from jax import lax
from jax.experimental import pallas as pl
from jax.experimental.pallas import tpu as pltpu
from jax.sharding import PartitionSpec as P

GROUPS = 32
NORM_EPS = 1e-6
MESH = pl.DeviceIdType.MESH
BF = jnp.bfloat16
F32 = jnp.float32
RING = 6


def make_kernel(group_size, height, width, channels):
    C = channels
    NT = C // 256
    FR = height * width
    assert height == 4
    elem_count = float(group_size * 2 * FR * (C // GROUPS))
    units_conv = 3 * NT
    units_all = 4 * units_conv

    def body(latent, conv_w, conv_b_in, norm_g_in, norm_b_in, attn_w, attn_b_in, out,
             conv_b, norm_g, norm_b, attn_b, wbuf, awbuf, xs0, xs1, xs2, xs3, buf, halo, acc, qkv, stat, norm,
             psem, wsem, awsem, insem, hsend, hrecv, ssend, srecv):
        me = lax.axis_index("time")
        xs = (xs0, xs1, xs2, xs3)
        xres = buf.at[0]

        def weight_copies(u):
            conv = u // units_conv
            rest = lax.rem(u, units_conv)
            tap_t = 2 - rest // NT
            tile = lax.rem(rest, NT)
            slot = lax.rem(u, RING)
            return [pltpu.make_async_copy(
                conv_w.at[conv, tap_t, d, :, :, pl.ds(pl.multiple_of(tile * 256, 256), 256)],
                wbuf.at[slot, d], wsem.at[slot, d]) for d in range(3)]

        def attn_weight_copy():
            return pltpu.make_async_copy(attn_w, awbuf, awsem)

        def in_copy(n):
            return pltpu.make_async_copy(latent.at[:, pl.ds(n * 256, 256)], xres.at[n], insem.at[n])

        def halo_copy(conv, n, f):
            return pltpu.make_async_remote_copy(
                src_ref=buf.at[lax.rem(conv, 2), n, pl.ds(f * FR, FR)],
                dst_ref=halo.at[conv, n, pl.ds(f * FR, FR)],
                send_sem=hsend.at[conv, n, f], recv_sem=hrecv.at[conv, n, f],
                device_id={"time": lax.rem(me + 1, group_size)}, device_id_type=MESH)

        def first_copy(conv, n, f):
            return pltpu.make_async_copy(
                buf.at[lax.rem(conv, 2), n, pl.ds(0, FR)], halo.at[conv, n, pl.ds(f * FR, FR)], hrecv.at[conv, n, f])

        def halo_start(conv):
            @pl.when(me < group_size - 1)
            def _():
                for f in (1, 0):
                    for n in range(NT):
                        halo_copy(conv, n, f).start()

            @pl.when(me == 0)
            def _():
                for f in (1, 0):
                    for n in range(NT):
                        first_copy(conv, n, f).start()

        def halo_wait(conv, f):
            @pl.when(me == 0)
            def _():
                for n in range(NT):
                    first_copy(conv, n, f).wait()

            @pl.when(me > 0)
            def _():
                for n in range(NT):
                    halo_copy(conv, n, f).wait_recv()

        def halo_wait_send(conv):
            @pl.when(me < group_size - 1)
            def _():
                for n in range(NT):
                    for f in (1, 0):
                        halo_copy(conv, n, f).wait_send()

        def stat_copy(g, p):
            return pltpu.make_async_remote_copy(
                src_ref=stat.at[g, me], dst_ref=stat.at[g, me],
                send_sem=ssend.at[g, p], recv_sem=srecv.at[g, p],
                device_id={"time": lax.rem(me + p, group_size)}, device_id_type=MESH)

        def weights_start(lo, hi):
            for u in range(lo, hi):
                for w in weight_copies(u):
                    w.start()

        small = [pltpu.make_async_copy(a, b, psem.at[i]) for i, (a, b) in enumerate(
            ((conv_b_in, conv_b), (norm_g_in, norm_g), (norm_b_in, norm_b), (attn_b_in, attn_b)))]
        for n in range(NT):
            in_copy(n).start()
        for p in small:
            p.start()

        barrier = pltpu.get_barrier_semaphore()
        for p in range(1, group_size):
            pl.semaphore_signal(barrier, inc=1, device_id={"time": lax.rem(me + p, group_size)}, device_id_type=MESH)

        def tile_cols(n):
            return pl.ds(n * 256 if isinstance(n, int) else pl.multiple_of(n * 256, 256), 256)

        def put_stats(g, n, s1, s2):
            stat[g, me, 0:1, tile_cols(n)] = jnp.sum(s1, axis=0, keepdims=True)
            stat[g, me, 1:2, tile_cols(n)] = jnp.sum(s2, axis=0, keepdims=True)

        def fold(v):
            return jnp.sum(v.reshape(v.shape[0] // 8, 8, v.shape[1]), axis=0)

        lane = lax.broadcasted_iota(jnp.int32, (2, 128), 1)

        def group_totals(v):
            size = C // GROUPS
            parts = [v[:, i * 128:(i + 1) * 128] for i in range(C // 128)]
            done = [jnp.zeros((2, 128), F32) for _ in parts]
            for q in range(GROUPS):
                lo, hi = q * size, (q + 1) * size
                inside = [(i, (lane >= lo - i * 128) & (lane < hi - i * 128)) for i in range(lo // 128, (hi - 1) // 128 + 1)]
                picked = sum(jnp.where(m, parts[i], 0.0) for i, m in inside)
                total = jnp.sum(picked, axis=1, keepdims=True)
                for i, m in inside:
                    done[i] = jnp.where(m, total, done[i])
            return jnp.concatenate(done, axis=1)

        def exchange(g, then=None):
            for p in range(1, group_size):
                stat_copy(g, p).start()
            if then is not None:
                then()
            for p in range(1, group_size):
                stat_copy(g, p).wait_recv()
            total = stat[g, 0]
            for r in range(1, group_size):
                total = total + stat[g, r]
            for p in range(1, group_size):
                stat_copy(g, p).wait_send()
            s = group_totals(total)
            mean = s[0:1] / elem_count
            var = s[1:2] / elem_count - mean * mean
            norm[0:1] = mean
            norm[1:2] = lax.rsqrt(var + NORM_EPS) * norm_g[pl.ds(g, 1)]
            norm[2:3] = norm_b[pl.ds(g, 1)]

        def normed(v, k):
            cols = pl.ds(k * 256, 256)
            return (v.astype(F32) - norm[0:1, cols]) * norm[1:2, cols] + norm[2:3, cols]

        row_id = lax.broadcasted_iota(jnp.int32, (width, 256), 0)

        def activate(src, slot, f, k):
            for row in range(height):
                rows = slice(row * width, (row + 1) * width)
                z = normed(src[k, f * FR + row * width:f * FR + (row + 1) * width, :], k)
                z = z * lax.logistic(z)
                at = k * 3 * 256
                xs[slot][rows, at:at + 256] = jnp.where(row_id == 0, 0.0, pltpu.roll(z, 1, 0)).astype(BF)
                xs[slot][rows, at + 256:at + 512] = z.astype(BF)
                xs[slot][rows, at + 512:at + 768] = jnp.where(row_id == width - 1, 0.0, pltpu.roll(z, width - 1, 0)).astype(BF)

        def trip(slot, tap_t, n):
            for d in ((1, 0, 2) if tap_t == 2 else (0, 2, 1)):
                w = jnp.concatenate([wbuf[slot, d, e, k * 256:(k + 1) * 256, :] for k in range(NT) for e in range(3)], axis=0)
                rows = FR if d == 1 else FR - width
                lo, dst = {0: (0, width), 1: (0, 0), 2: (width, 0)}[d]
                order = (0, 1) if tap_t == 2 else (1, 0)
                lhs = jnp.concatenate([xs[tap_t + f][lo:lo + rows, :] for f in order], axis=0)
                r = jnp.dot(lhs, w, preferred_element_type=F32)
                if d == 1 and tap_t == 2:
                    acc[n] = r
                else:
                    for at, f in enumerate(order):
                        acc[n, f * FR + dst:f * FR + dst + rows, :] += r[at * rows:(at + 1) * rows]

        def epilogue(c, n, g):
            odd = lax.rem(c, 2)
            bias = conv_b[pl.ds(c, 1), n * 256:(n + 1) * 256]
            keep = odd.astype(F32)
            s1 = jnp.zeros((8, 256), F32)
            s2 = jnp.zeros((8, 256), F32)
            for j in range(2 * height):
                rows = slice(j * width, (j + 1) * width)
                h = (acc[n, rows, :] + bias).astype(BF).astype(F32)
                h = (xres[n, rows, :].astype(F32) * keep + h).astype(BF)
                buf[1 - odd, n, rows, :] = h
                out[rows, n * 256:(n + 1) * 256] = h
                hf = h.astype(F32)
                s1 = s1 + fold(hf)
                s2 = s2 + fold(hf * hf)
            put_stats(g, n, s1, s2)

        def conv(c):
            base = c * units_conv
            g_in = c + c // 2
            src = buf.at[lax.rem(c, 2)]

            def behind_sums():
                halo_start(c)
                for n in range(NT):
                    for w in weight_copies(base + NT + n):
                        w.start()

            exchange(g_in, behind_sums)

            for tap_t in (2, 1, 0):
                first = base + (2 - tap_t) * NT
                for n in range(NT):
                    for w in weight_copies(first + n):
                        w.wait()
                if tap_t < 2:
                    halo_wait(c, tap_t)
                if tap_t == 0:
                    halo_wait_send(c)

                @pl.when(me < group_size)
                def _():
                    if tap_t == 2:
                        for k in range(NT):
                            for f in range(2):
                                activate(src, 2 + f, f, k)
                    else:
                        for k in range(NT):
                            activate(halo.at[c], tap_t, tap_t, k)
                    for n in range(NT):
                        trip(lax.rem(first + n, RING), tap_t, n)
                        if tap_t == 0:
                            epilogue(c, n, g_in + 1)

                if tap_t == 1:
                    @pl.when(c == 0)
                    def _():
                        attn_weight_copy().start()
                for n in range(NT if tap_t > 0 else 0):
                    @pl.when(first + n + RING < units_all)
                    def _():
                        for w in weight_copies(first + n + RING):
                            w.start()

        def attention(g):
            attn_weight_copy().wait()
            for k in range(NT):
                for j in range(2 * height):
                    at = slice(j * width, (j + 1) * width)
                    qkv[3, at, k * 256:(k + 1) * 256] = normed(xres[k, at, :], k).astype(BF)
            for w in range(3):
                for n in range(NT):
                    cols = slice(n * 256, (n + 1) * 256)
                    for f in range(2):
                        rows = slice(f * FR, (f + 1) * FR)
                        v = jnp.dot(qkv[3, rows, :], awbuf[w, :, cols], preferred_element_type=F32) + attn_b[w:w + 1, cols]
                        qkv[w, rows, cols] = v.astype(BF)
            for f in range(2):
                rows = slice(f * FR, (f + 1) * FR)
                scores = lax.dot_general(qkv[0, rows, :], qkv[1, rows, :], (((1,), (1,)), ((), ())), preferred_element_type=F32)
                scores = scores * (C ** -0.5)
                e = jnp.exp(scores - jnp.max(scores, axis=1, keepdims=True))
                probs = (e / jnp.sum(e, axis=1, keepdims=True)).astype(BF)
                qkv[3, rows, :] = jnp.dot(probs, qkv[2, rows, :], preferred_element_type=F32).astype(BF)
            for n in range(NT):
                cols = slice(n * 256, (n + 1) * 256)
                s1 = jnp.zeros((8, 256), F32)
                s2 = jnp.zeros((8, 256), F32)
                for f in range(2):
                    rows = slice(f * FR, (f + 1) * FR)
                    h = (jnp.dot(qkv[3, rows, :], awbuf[3, :, cols], preferred_element_type=F32) + attn_b[3:4, cols]).astype(BF)
                    h = (xres[n, rows, :].astype(F32) + h.astype(F32)).astype(BF)
                    xres[n, rows, :] = h
                    hf = h.astype(F32)
                    s1 = s1 + fold(hf)
                    s2 = s2 + fold(hf * hf)
                put_stats(g + 1, n, s1, s2)

        for n in range(NT):
            in_copy(n).wait()
        weights_start(0, NT)
        for p in small:
            p.wait()
        pl.semaphore_wait(barrier, group_size - 1)
        for n in range(NT):
            def in_stats(j, carry):
                v = xres[n, pl.ds(pl.multiple_of(j * width, width), width), :].astype(F32)
                return carry[0] + fold(v), carry[1] + fold(v * v)

            s1, s2 = lax.fori_loop(0, 2 * height, in_stats, (jnp.zeros((8, 256), F32), jnp.zeros((8, 256), F32)))
            put_stats(0, n, s1, s2)
        def layer(c, carry):
            conv(c)

            @pl.when(c == 1)
            def _():
                exchange(2)
                attention(2)
            return carry

        lax.fori_loop(0, 4, layer, 0)

    scratch = [
        pltpu.VMEM((4, C), F32),
        pltpu.VMEM((5, C), F32),
        pltpu.VMEM((5, C), F32),
        pltpu.VMEM((4, C), F32),
        pltpu.VMEM((RING, 3, 3, C, 256), BF),
        pltpu.VMEM((4, C, C), BF),
        pltpu.VMEM((FR, 3 * C), BF),
        pltpu.VMEM((FR, 3 * C), BF),
        pltpu.VMEM((FR, 3 * C), BF),
        pltpu.VMEM((FR, 3 * C), BF),
        pltpu.VMEM((2, NT, 2 * FR, 256), BF),
        pltpu.VMEM((4, NT, 2 * FR, 256), BF),
        pltpu.VMEM((NT, 2 * FR, 256), F32),
        pltpu.VMEM((4, 2 * FR, C), BF),
        pltpu.VMEM((6, group_size, 2, C), F32),
        pltpu.VMEM((8, C), F32),
        pltpu.SemaphoreType.DMA((4,)),
        pltpu.SemaphoreType.DMA((RING, 3)),
        pltpu.SemaphoreType.DMA,
        pltpu.SemaphoreType.DMA((NT,)),
        pltpu.SemaphoreType.DMA((4, NT, 2)),
        pltpu.SemaphoreType.DMA((4, NT, 2)),
        pltpu.SemaphoreType.DMA((5, group_size)),
        pltpu.SemaphoreType.DMA((5, group_size)),
    ]
    return body, scratch


def solution(mesh):
    group_size = mesh.shape["time"]
    video_spec = P(("batch", "time"), None, None, None)

    def device_body(latent, conv_w, conv_b, norm_g, norm_b, attn_w, attn_b):
        frames, height, width, channels = latent.shape
        body, scratch = make_kernel(group_size, height, width, channels)
        pinned = [pltpu.with_memory_space_constraint(p, pltpu.HBM) for p in (conv_b, norm_g, norm_b, attn_b)]
        hbm = pl.BlockSpec(memory_space=pltpu.HBM)
        out = pl.pallas_call(
            body,
            out_shape=jax.ShapeDtypeStruct((frames * height * width, channels), BF),
            in_specs=[hbm] * 7,
            out_specs=pl.BlockSpec(memory_space=pltpu.VMEM),
            scratch_shapes=scratch,
            compiler_params=pltpu.CompilerParams(collective_id=0, has_side_effects=True, vmem_limit_bytes=52 * 1024 * 1024),
            name="mid_block",
        )(latent.reshape(frames * height * width, channels), conv_w, *pinned[:3], attn_w, pinned[3])
        return out.reshape(latent.shape)

    return jax.shard_map(device_body, mesh=mesh, in_specs=(video_spec, P(), P(), P(), P(), P(), P()), out_specs=video_spec, check_vma=False)
```
